32 devices in a mesh: tp: 4 (over z), cp: 2 (over x), dp: 4 (over y, core).
Axes of the slice: x: 2, y: 2, z: 4, core: 2. Of those that a mesh axis runs over, the one named last changes fastest.
Arguments:
- tokens: bfloat16 [2048, 7168], P(('dp', 'tp', 'cp')), parts along dimension 0, may hold values from -6 to 6
- router: bfloat16 [7168, 4], replicated, may hold values from -0.0625 to 0.0625
- gate_weight: bfloat16 [4, 7168, 1024], P('cp', None, 'tp'), may hold values from -0.0625 to 0.0625
- up_weight: bfloat16 [4, 7168, 1024], P('cp', None, 'tp'), may hold values from -0.0625 to 0.0625
- down_weight: bfloat16 [4, 1024, 7168], P('cp', 'tp'), may hold values from -0.1875 to 0.1875
- expert_ids: int32 [2048, 2], P(('dp', 'tp', 'cp')), parts along dimension 0, may hold values from 0 to 3, as said below
- slot_index: int32 [2048, 2], P(('dp', 'tp', 'cp')), parts along dimension 0, may hold values from -1 to 1, as said below
Outputs:
- moe_out: bfloat16 [2048, 7168], P(('dp', 'tp', 'cp')), parts along dimension 0
The draws below stay inside these ranges and needn't reach their ends.
There are 4 independent parts, one for each index of `dp`. The reference program is written for one: setup_inputs(seed, part) draws one part's arguments, and reference() takes and returns one part's arrays. A program takes and returns all parts, laid end to end along the dimension named above; an argument that names none is the same for every part. Nothing has to cross between parts.
Inputs may be any that keep to these rules, and one draw needn't show every extreme that they name: `expert_ids`: each row names 2 different experts in rising order; in every part one expert is named by 32 or more rows of every block. slot_index[t, k] is the number of earlier copies to expert expert_ids[t, k] within token t's block (rows in order, then k in order) when that is below 2, else -1.
All inputs are finite; a program needn't handle non-finite values.
Results may differ from the reference program's by a relative error of at most 0.012.
Values may be sent and summed in bfloat16 or wider, within the bound.
A program may use at most 64 MiB of HBM per device.

```python
import jax
import jax.numpy as jnp
from jax import lax

D = 7168
FF = 1024
TOP = 2
TOK_DEV = 64
CAP_DEV = 2
SPECIALIST_COUNT = 4
FF_DEV = 256
TOKENS = 512
N_TP = 4
N_CP = 2


def routing(key):
    blocks = N_TP * N_CP
    key_hot, key_noise, key_bias, key_rank = jax.random.split(key, 4)
    crowded_specialist = jax.random.randint(key_hot, (), 0, SPECIALIST_COUNT)
    normal_perturbation = jax.random.randint(key_noise, (blocks, TOK_DEV, SPECIALIST_COUNT), 0, 1 << 16)
    dispatcher_offset = jax.random.randint(key_bias, (blocks, 1, SPECIALIST_COUNT), 0, 1 << 15)
    order = jax.random.randint(key_rank, (blocks, TOK_DEV), 0, 1 << 20) * TOK_DEV + jnp.arange(TOK_DEV, dtype=jnp.int32)[None, :]
    ranking = jnp.argsort(jnp.argsort(order, axis=1, stable=True), axis=1, stable=True)
    preferred_specialist = ranking < TOK_DEV // 2
    uniform_samples = jnp.arange(SPECIALIST_COUNT, dtype=jnp.int32)
    preference_offset = jnp.where(preferred_specialist[:, :, None] & (uniform_samples[None, None, :] == crowded_specialist), 1 << 17, 0)
    dispatcher_logit = (normal_perturbation + dispatcher_offset + preference_offset) * SPECIALIST_COUNT + uniform_samples[None, None, :]
    top_values, top_ids = lax.top_k(dispatcher_logit, TOP)
    chosen_ids = jnp.sort(top_ids.astype(jnp.int32), axis=-1)
    onehot = (chosen_ids[:, :, :, None] == uniform_samples).astype(jnp.int32).reshape(blocks, TOK_DEV * TOP, SPECIALIST_COUNT)
    earlier = jnp.cumsum(onehot, axis=1) - onehot
    position = jnp.sum(earlier * onehot, axis=-1).reshape(blocks, TOK_DEV, TOP)
    slot_values = jnp.where(position < CAP_DEV, position, -1).astype(jnp.int32)
    return (chosen_ids.reshape(TOKENS, TOP), slot_values.reshape(TOKENS, TOP))


def draw_expert_ids(key, part):
    return routing(jax.random.fold_in(key, 11))[0]


def draw_slot_index(key, part):
    return routing(jax.random.fold_in(key, 11))[1]


def level_of(key, shape, cuts, least, largest):
    def one(axis_at, parts):
        draws = jax.random.uniform(jax.random.fold_in(jax.random.fold_in(key, 6), axis_at), (parts,), jnp.float32, least / len(cuts), largest / len(cuts))
        return jnp.repeat(jnp.exp(draws), shape[axis_at] // parts).reshape((-1,) + (1,) * (len(shape) - axis_at - 1))

    level = one(*cuts[0])
    for cut in cuts[1:]:
        level = level * one(*cut)
    return level


def gaussian(own_key, shape, width, limit, shards=(), kind=jnp.bfloat16):
    drawn = jax.random.normal(own_key, shape, jnp.float32) * width
    if len(shards) > 0:
        drawn = level_of(own_key, shape, shards, -0.22, 0.18) * drawn
    return jnp.clip(drawn, min=-limit, max=limit).astype(kind)


def setup_inputs(seed: int = 0, part: int = 0) -> dict:
    arg_keys = jax.random.split(jax.random.key(seed), 8)
    part_splits = jax.random.split(jax.random.fold_in(arg_keys[7], part), 8)
    return {
        "tokens": gaussian(part_splits[0], (TOKENS, D), 1.0, 6.0, ((0, 8),)),
        "router": gaussian(arg_keys[1], (D, SPECIALIST_COUNT), D ** -0.5, 0.0625),
        "gate_weight": gaussian(arg_keys[2], (SPECIALIST_COUNT, D, FF), D ** -0.5, 0.0625, ((0, 2), (2, 4))),
        "up_weight": gaussian(arg_keys[3], (SPECIALIST_COUNT, D, FF), D ** -0.5, 0.0625, ((0, 2), (2, 4))),
        "down_weight": gaussian(arg_keys[4], (SPECIALIST_COUNT, FF, D), FF ** -0.5, 0.1875, ((0, 2), (1, 4))),
        "expert_ids": draw_expert_ids(jax.random.fold_in(jax.random.fold_in(arg_keys[7], part), 71), part),
        "slot_index": draw_slot_index(jax.random.fold_in(jax.random.fold_in(arg_keys[7], part), 71), part),
    }


route_scale = 2.5


def reference(tokens, router, gate_weight, up_weight, down_weight, expert_ids, slot_index):
    logits = jnp.dot(tokens, router, preferred_element_type=jnp.float32)
    affinity = jax.nn.sigmoid(logits)
    chosen = jnp.take_along_axis(affinity, expert_ids, axis=1)
    gate_share = route_scale * chosen / jnp.sum(chosen, axis=1, keepdims=True)
    blocks = N_TP * N_CP
    token_block = (jnp.arange(TOKENS) // TOK_DEV).astype(jnp.int32)
    slot_total = SPECIALIST_COUNT * blocks * CAP_DEV
    destination = jnp.where(slot_index >= 0, expert_ids * (blocks * CAP_DEV) + token_block[:, None] * CAP_DEV + slot_index, slot_total).astype(jnp.int32)
    buffer = jnp.zeros((slot_total + 1, D), jnp.bfloat16)
    buffer = buffer.at[destination.reshape(-1)].set(jnp.repeat(tokens, TOP, axis=0))
    dispatched = buffer[:slot_total].reshape(SPECIALIST_COUNT, blocks * CAP_DEV, D)

    def one_expert(pieces):
        expert_rows, w_gate, w_up, w_down = pieces
        gate_part = jnp.dot(expert_rows, w_gate, preferred_element_type=jnp.float32)
        up_part = jnp.dot(expert_rows, w_up, preferred_element_type=jnp.float32)
        hidden = (jax.nn.silu(gate_part) * up_part).astype(jnp.bfloat16)
        grouped = hidden.reshape(blocks * CAP_DEV, N_TP, FF_DEV).astype(jnp.float32)
        down_groups = w_down.reshape(N_TP, FF_DEV, D).astype(jnp.float32)
        partial_value = jnp.einsum("mgf,gfd->gmd", grouped, down_groups).astype(jnp.bfloat16)
        partial_value = lax.optimization_barrier(partial_value)
        return jnp.sum(partial_value.astype(jnp.float32), axis=0)

    expert_out = lax.map(one_expert, (dispatched, gate_weight, up_weight, down_weight))
    flat_index = (expert_ids * (blocks * CAP_DEV) + token_block[:, None] * CAP_DEV + jnp.maximum(slot_index, 0)).astype(jnp.int32)
    picked = expert_out.reshape(slot_total, D)[flat_index]
    weight = jnp.where(slot_index >= 0, gate_share, jnp.float32(0.0))
    return jnp.sum(picked * weight[:, :, None], axis=1).astype(jnp.bfloat16)
```

```python
import functools

import jax
import jax.numpy as jnp
from jax import lax
from jax.experimental import pallas as pl
from jax.experimental.pallas import tpu as pltpu
from jax.sharding import PartitionSpec as P

CAP_DEV = 2
ROUTE_SCALE = 2.5
CHUNKS = 1
SPLIT = 4
MESH = pl.DeviceIdType.MESH
NT = (((1,), (1,)), ((), ()))


def rows_of(pieces):
    return jnp.concatenate([p.astype(jnp.float32) for p in pieces], axis=0).astype(jnp.bfloat16)


def flip(index, bits):
    for b in range(bits.bit_length()):
        if (bits >> b) & 1:
            index = index + (1 - 2 * lax.rem(index // (1 << b), 2)) * (1 << b)
    return index


def exchange_kernel(
    n_tp, n_cp, nc,
    tok_hbm, rt_hbm, ids_hbm, slot_hbm, wg_hbm, wu_hbm, wd_hbm,
    pr, mix_ref,
    ids_ref, slot_ref, tok, rt, wg, wu, wd, xs, xr, ps,
    in_sem, wsem, s1, r1, s2, r2,
):
    n = n_tp * n_cp
    my_z, my_x = lax.axis_index("tp"), lax.axis_index("cp")
    me = my_z * n_cp + my_x
    local, width, ff = wg.shape
    dc = width // nc
    slots = n_cp * local * CAP_DEV
    pow2 = n & (n - 1) == 0
    order = list(range(n - 1, 0, -1))

    def peer(j):
        return flip(me, j) if pow2 else lax.rem(me + j, n)

    def source(j):
        return flip(me, j) if pow2 else lax.rem(me + n - j, n)

    def device(other):
        return {"tp": other // n_cp, "cp": lax.rem(other, n_cp)}

    index_copies = [
        pltpu.make_async_copy(ids_hbm, ids_ref, in_sem.at[nc + 1]),
        pltpu.make_async_copy(slot_hbm, slot_ref, in_sem.at[nc + 2]),
    ]
    for copy in index_copies:
        copy.start()
    tok_copies = []
    for c in range(nc):
        cols = pl.ds(c * dc, dc)
        copy = pltpu.make_async_copy(tok_hbm.at[:, cols], tok.at[:, cols], in_sem.at[c])
        copy.start()
        tok_copies.append(copy)
    rt_copy = pltpu.make_async_copy(rt_hbm, rt, in_sem.at[nc])
    rt_copy.start()

    barrier = pltpu.get_barrier_semaphore()
    for j in order:
        pl.semaphore_signal(barrier, inc=1, device_id=device(peer(j)), device_id_type=MESH)

    up_copies, down_copies = {}, {}
    for e in range(local):
        for c in range(nc):
            cols = pl.ds(c * dc, dc)
            pair = [
                pltpu.make_async_copy(wg_hbm.at[e, cols, :], wg.at[e, cols, :], wsem.at[0, e, c]),
                pltpu.make_async_copy(wu_hbm.at[e, cols, :], wu.at[e, cols, :], wsem.at[1, e, c]),
            ]
            for copy in pair:
                copy.start()
            up_copies[e, c] = pair
        for c in range(nc):
            cols = pl.ds(c * dc, dc)
            copy = pltpu.make_async_copy(wd_hbm.at[e, :, cols], wd.at[e, :, cols], wsem.at[2, e, c])
            copy.start()
            down_copies[e, c] = copy

    for copy in index_copies:
        copy.wait()
    ids0, ids1 = ids_ref[0:1, :], ids_ref[1:2, :]
    slot0, slot1 = slot_ref[0:1, :], slot_ref[1:2, :]
    target0 = jnp.where(slot0 >= 0, ids0 * CAP_DEV + slot0, -1)
    target1 = jnp.where(slot1 >= 0, ids1 * CAP_DEV + slot1, -1)
    row = lax.broadcasted_iota(jnp.int32, (slots, ids0.shape[1]), 0)
    placing = jnp.where((row == target0) | (row == target1), 1.0, 0.0).astype(jnp.bfloat16)

    def dispatch(e, c):
        for j in order:
            other = peer(j)
            pltpu.make_async_remote_copy(
                src_ref=xs.at[e, c, lax.rem(other, n_cp)],
                dst_ref=xr.at[e, c, me],
                send_sem=s1,
                recv_sem=r1.at[e, c],
                device_id=device(other),
                device_id_type=MESH,
            ).start()
        xr[e, c, me] = xs[e, c, my_x]

    for c in range(nc):
        tok_copies[c].wait()
        cols = pl.ds(c * dc, dc)
        outgoing = jnp.dot(placing, tok[:, cols], preferred_element_type=jnp.float32)
        for x in range(n_cp):
            for e in range(local):
                at = (x * local + e) * CAP_DEV
                xs[e, c, x] = outgoing[at:at + CAP_DEV].astype(jnp.bfloat16)
        if c == 0:
            pl.semaphore_wait(barrier, n - 1)
        dispatch(0, c)
    for e in range(1, local):
        for c in range(nc):
            dispatch(e, c)

    rt_copy.wait()
    logits = lax.dot_general(rt[...], tok[...], NT, preferred_element_type=jnp.float32)
    affinity = 1.0 / (1.0 + jnp.exp(-logits))
    erow = lax.broadcasted_iota(jnp.int32, logits.shape, 0)
    chosen0 = jnp.sum(jnp.where(erow == ids0, affinity, 0.0), axis=0, keepdims=True)
    chosen1 = jnp.sum(jnp.where(erow == ids1, affinity, 0.0), axis=0, keepdims=True)
    total = chosen0 + chosen1
    share0 = ROUTE_SCALE * chosen0 / total
    share1 = ROUTE_SCALE * chosen1 / total
    wide = lax.broadcasted_iota(jnp.int32, (local * n * CAP_DEV, ids0.shape[1]), 0)
    which = lax.rem(wide // CAP_DEV, n_cp) * local + wide // (n * CAP_DEV)
    wide = which * CAP_DEV + lax.rem(wide, CAP_DEV)
    mix = jnp.where(wide == target0, share0, 0.0) + jnp.where(wide == target1, share1, 0.0)
    mix = mix.T
    mix_hi = mix.astype(jnp.bfloat16)
    mix_lo = (mix - mix_hi.astype(jnp.float32)).astype(jnp.bfloat16)
    mix_ref[...] = jnp.concatenate([mix_hi, mix_lo], axis=0)

    def drain(ref, sem):
        pltpu.make_async_copy(ref, ref, sem).wait()

    for e in range(local):
        gate = jnp.zeros((n * CAP_DEV, ff), jnp.float32)
        up = jnp.zeros((n * CAP_DEV, ff), jnp.float32)
        for c in range(nc):
            cols = pl.ds(c * dc, dc)
            for copy in up_copies[e, c]:
                copy.wait()
            drain(xr.at[e, c, pl.ds(0, n - 1)], r1.at[e, c])
            x = rows_of([xr[e, c, i] for i in range(n)])
            gate += jnp.dot(x, wg[e, cols, :], preferred_element_type=jnp.float32)
            up += jnp.dot(x, wu[e, cols, :], preferred_element_type=jnp.float32)
        hidden = (gate / (1.0 + jnp.exp(-gate)) * up).astype(jnp.bfloat16)
        for c in range(nc):
            cols = pl.ds(c * dc, dc)
            down_copies[e, c].wait()
            part = jnp.dot(hidden, wd[e, :, cols], preferred_element_type=jnp.float32)
            for i in range(n):
                ps[e, c, i] = part[i * CAP_DEV:(i + 1) * CAP_DEV].astype(jnp.bfloat16)
            for other in range(n):
                @pl.when(other != me)
                def _():
                    pltpu.make_async_remote_copy(
                        src_ref=ps.at[e, c, other],
                        dst_ref=pr.at[e, c, me],
                        send_sem=s2,
                        recv_sem=r2,
                        device_id=device(jnp.int32(other)),
                        device_id_type=MESH,
                    ).start()
            pr[e, c, me] = ps[e, c, me]
    drain(xr.at[:, :, pl.ds(0, n - 1)], s1)
    drain(pr.at[:, :, pl.ds(0, n - 1)], s2)
    drain(pr.at[:, :, pl.ds(0, n - 1)], r2)


def combine_kernel(pr, mix_ref, out_hbm, ob, osem):
    local, nc, n, cap, dc = pr.shape
    mix = mix_ref[...]
    half = mix.shape[0] // 2
    part = dc // SPLIT
    outs = []
    for c in range(nc):
        for p in range(SPLIT):
            at = pl.ds(p * part, part)
            cols = pl.ds(c * dc + p * part, part)
            rows = rows_of([pr[e, c, i, :, at] for e in range(local) for i in range(n)])
            both = jnp.dot(mix, rows, preferred_element_type=jnp.float32)
            ob[:, cols] = (both[:half] + both[half:]).astype(jnp.bfloat16)
            copy = pltpu.make_async_copy(ob.at[:, cols], out_hbm.at[:, cols], osem.at[c, p])
            copy.start()
            outs.append(copy)
    for copy in outs:
        copy.wait()


def body(n_tp, n_cp, tokens, router, gate_weight, up_weight, down_weight, expert_ids, slot_index):
    n = n_tp * n_cp
    rows, width = tokens.shape
    local, _, ff = gate_weight.shape
    nc = CHUNKS if n <= 16 else 1
    dc = width // nc
    anywhere = pl.BlockSpec(memory_space=pl.ANY)
    resident = pl.BlockSpec(memory_space=pltpu.VMEM)
    bf16 = jnp.bfloat16
    dma = pltpu.SemaphoreType.DMA
    slab = (local, nc, n, CAP_DEV, dc)
    pr, mix = pl.pallas_call(
        functools.partial(exchange_kernel, n_tp, n_cp, nc),
        out_shape=[
            pltpu.VMEM(slab, bf16),
            pltpu.VMEM((2 * rows, local * n * CAP_DEV), bf16),
        ],
        in_specs=[anywhere] * 7,
        out_specs=[resident, resident],
        scratch_shapes=[
            pltpu.VMEM((expert_ids.shape[1], rows), jnp.int32),
            pltpu.VMEM((slot_index.shape[1], rows), jnp.int32),
            pltpu.VMEM((rows, width), bf16),
            pltpu.VMEM((router.shape[1], width), bf16),
            pltpu.VMEM((local, width, ff), bf16),
            pltpu.VMEM((local, width, ff), bf16),
            pltpu.VMEM((local, ff, width), bf16),
            pltpu.VMEM((local, nc, n_cp, CAP_DEV, dc), bf16),
            pltpu.VMEM(slab, bf16),
            pltpu.VMEM(slab, bf16),
            dma((nc + 3,)),
            dma((3, local, nc)),
            dma,
            dma((local, nc)),
            dma,
            dma,
        ],
        compiler_params=pltpu.CompilerParams(
            collective_id=0, has_side_effects=True, vmem_limit_bytes=60 * 1024 * 1024
        ),
    )(tokens, router.T, expert_ids.T, slot_index.T, gate_weight, up_weight, down_weight)
    return pl.pallas_call(
        combine_kernel,
        out_shape=jax.ShapeDtypeStruct((rows, width), bf16),
        in_specs=[resident, resident],
        out_specs=anywhere,
        scratch_shapes=[
            pltpu.VMEM((rows, width), bf16),
            dma((nc, SPLIT)),
        ],
        compiler_params=pltpu.CompilerParams(vmem_limit_bytes=8 * 1024 * 1024),
    )(pr, mix)


def solution(mesh):
    in_specs = (
        P(("dp", "tp", "cp"), None),
        P(),
        P("cp", None, "tp"),
        P("cp", None, "tp"),
        P("cp", "tp", None),
        P(("dp", "tp", "cp"), None),
        P(("dp", "tp", "cp"), None),
    )
    out_specs = P(("dp", "tp", "cp"), None)
    step = functools.partial(body, mesh.shape["tp"], mesh.shape["cp"])
    return jax.shard_map(step, mesh=mesh, in_specs=in_specs, out_specs=out_specs, check_vma=False)
```

```python
import functools

import jax
import jax.numpy as jnp
from jax import lax
from jax.experimental import pallas as pl
from jax.experimental.pallas import tpu as pltpu
from jax.sharding import PartitionSpec as P

CAP_DEV = 2
ROUTE_SCALE = 2.5
CHUNKS = 1
SPLIT = 4
MESH = pl.DeviceIdType.MESH
NT = (((1,), (1,)), ((), ()))


def rows_of(pieces):
    return jnp.concatenate([p.astype(jnp.float32) for p in pieces], axis=0).astype(jnp.bfloat16)


def flip(index, bits):
    for b in range(bits.bit_length()):
        if (bits >> b) & 1:
            index = index + (1 - 2 * lax.rem(index // (1 << b), 2)) * (1 << b)
    return index


def exchange_kernel(
    n_tp, n_cp, nc,
    tok_hbm, rt_hbm, ids_hbm, slot_hbm, wg_hbm, wu_hbm, wd_hbm,
    pr, mix_ref,
    ids_ref, slot_ref, tok, rt, wg, wu, wd, xs, xr, ps,
    in_sem, wsem, s1, r1, fs, fr, s2, r2,
):
    n = n_tp * n_cp
    my_z, my_x = lax.axis_index("tp"), lax.axis_index("cp")
    me = my_z * n_cp + my_x
    local, width, ff = wg.shape
    dc = width // nc
    slots = n_cp * local * CAP_DEV
    pow2 = n & (n - 1) == 0
    h = n_tp // 2 if n_tp % 2 == 0 and n_tp > 2 else n_tp
    inner = (h - 1, h)
    order = list(range(n - 1, 0, -1))

    def peer(j):
        return flip(me, j) if pow2 else lax.rem(me + j, n)

    def source(j):
        return flip(me, j) if pow2 else lax.rem(me + n - j, n)

    def device(other):
        return {"tp": other // n_cp, "cp": lax.rem(other, n_cp)}

    def drain(ref, sem):
        pltpu.make_async_copy(ref, ref, sem).wait()

    index_copies = [
        pltpu.make_async_copy(ids_hbm, ids_ref, in_sem.at[nc + 1]),
        pltpu.make_async_copy(slot_hbm, slot_ref, in_sem.at[nc + 2]),
    ]
    for copy in index_copies:
        copy.start()
    tok_copies = []
    for c in range(nc):
        cols = pl.ds(c * dc, dc)
        copy = pltpu.make_async_copy(tok_hbm.at[:, cols], tok.at[:, cols], in_sem.at[c])
        copy.start()
        tok_copies.append(copy)
    rt_copy = pltpu.make_async_copy(rt_hbm, rt, in_sem.at[nc])
    rt_copy.start()

    barrier = pltpu.get_barrier_semaphore()
    for j in order:
        pl.semaphore_signal(barrier, inc=1, device_id=device(peer(j)), device_id_type=MESH)

    up_copies, down_copies = {}, {}
    for e in range(local):
        for c in range(nc):
            cols = pl.ds(c * dc, dc)
            pair = [
                pltpu.make_async_copy(wg_hbm.at[e, cols, :], wg.at[e, cols, :], wsem.at[0, e, c]),
                pltpu.make_async_copy(wu_hbm.at[e, cols, :], wu.at[e, cols, :], wsem.at[1, e, c]),
            ]
            for copy in pair:
                copy.start()
            up_copies[e, c] = pair
        for c in range(nc):
            cols = pl.ds(c * dc, dc)
            copy = pltpu.make_async_copy(wd_hbm.at[e, :, cols], wd.at[e, :, cols], wsem.at[2, e, c])
            copy.start()
            down_copies[e, c] = copy

    for copy in index_copies:
        copy.wait()
    ids0, ids1 = ids_ref[0:1, :], ids_ref[1:2, :]
    slot0, slot1 = slot_ref[0:1, :], slot_ref[1:2, :]
    target0 = jnp.where(slot0 >= 0, ids0 * CAP_DEV + slot0, -1)
    target1 = jnp.where(slot1 >= 0, ids1 * CAP_DEV + slot1, -1)
    row = lax.broadcasted_iota(jnp.int32, (slots, ids0.shape[1]), 0)
    placing = jnp.where((row == target0) | (row == target1), 1.0, 0.0).astype(jnp.bfloat16)

    half = my_z // h
    gateway = (my_z == inner[0]) | (my_z == inner[-1])
    pair = range(n_tp // h)

    def place(e, c, z, x, recv_sem):
        pltpu.make_async_remote_copy(
            src_ref=xs.at[e, c, x],
            dst_ref=xr.at[e, c, me],
            send_sem=s1,
            recv_sem=recv_sem,
            device_id={"tp": jnp.int32(z), "cp": jnp.int32(x)},
            device_id_type=MESH,
        ).start()

    def dispatch(e, c):
        for b in pair:
            for z in [inner[b]] + [z for z in range(b * h, b * h + h) if z != inner[b]]:
                if h == n_tp:
                    continue
                @pl.when((half != b) if z == inner[b] else (half != b) & gateway)
                def _():
                    for x in range(n_cp):
                        place(e, c, z, x, fr.at[e, c, lax.rem(me, h * n_cp)])
        for z in range(n_tp):
            for x in range(n_cp):
                @pl.when((half == z // h) & (me != z * n_cp + x))
                def _():
                    place(e, c, z, x, r1.at[e, c])
        xr[e, c, me] = xs[e, c, my_x]

    def across(k):
        return (1 - half) * (h * n_cp) + k

    def forward(e, c):
        for b in pair if h < n_tp else ():
            @pl.when(my_z == inner[b])
            def _():
                far = [z for z in range((1 - b) * h, (1 - b) * h + h) if z != inner[1 - b]]
                near = [z for z in range(b * h, b * h + h) if z != inner[b]]
                for k in [z * n_cp + x for z in far for x in range(n_cp)]:
                    drain(xr.at[e, c, k], fr.at[e, c, k % (h * n_cp)])
                    for m, z in enumerate(near):
                        pltpu.make_async_remote_copy(
                            src_ref=xr.at[e, c, k],
                            dst_ref=xr.at[e, c, k],
                            send_sem=fs.at[m],
                            recv_sem=fr.at[e, c, k % (h * n_cp)],
                            device_id={"tp": jnp.int32(z), "cp": my_x},
                            device_id_type=MESH,
                        ).start()

    def collect(e, c):
        if h * n_cp > 1:
            drain(xr.at[e, c, pl.ds(0, h * n_cp - 1)], r1.at[e, c])
        for b in pair if h < n_tp else ():
            other = range((1 - b) * h, (1 - b) * h + h)
            @pl.when(half == b)
            def _():
                for x in range(n_cp):
                    k = inner[1 - b] * n_cp + x
                    drain(xr.at[e, c, k], fr.at[e, c, k % (h * n_cp)])
            @pl.when((half == b) & jnp.logical_not(gateway))
            def _():
                for k in [z * n_cp + x for z in other if z != inner[1 - b] for x in range(n_cp)]:
                    drain(xr.at[e, c, k], fr.at[e, c, k % (h * n_cp)])

    for c in range(nc):
        tok_copies[c].wait()
        cols = pl.ds(c * dc, dc)
        outgoing = jnp.dot(placing, tok[:, cols], preferred_element_type=jnp.float32)
        for x in range(n_cp):
            for e in range(local):
                at = (x * local + e) * CAP_DEV
                xs[e, c, x] = outgoing[at:at + CAP_DEV].astype(jnp.bfloat16)
        if c == 0:
            pl.semaphore_wait(barrier, n - 1)
        dispatch(0, c)
    for e in range(1, local):
        for c in range(nc):
            dispatch(e, c)

    rt_copy.wait()
    logits = lax.dot_general(rt[...], tok[...], NT, preferred_element_type=jnp.float32)
    affinity = 1.0 / (1.0 + jnp.exp(-logits))
    erow = lax.broadcasted_iota(jnp.int32, logits.shape, 0)
    chosen0 = jnp.sum(jnp.where(erow == ids0, affinity, 0.0), axis=0, keepdims=True)
    chosen1 = jnp.sum(jnp.where(erow == ids1, affinity, 0.0), axis=0, keepdims=True)
    total = chosen0 + chosen1
    share0 = ROUTE_SCALE * chosen0 / total
    share1 = ROUTE_SCALE * chosen1 / total
    wide = lax.broadcasted_iota(jnp.int32, (local * n * CAP_DEV, ids0.shape[1]), 0)
    which = lax.rem(wide // CAP_DEV, n_cp) * local + wide // (n * CAP_DEV)
    wide = which * CAP_DEV + lax.rem(wide, CAP_DEV)
    mix = jnp.where(wide == target0, share0, 0.0) + jnp.where(wide == target1, share1, 0.0)
    mix = mix.T
    mix_hi = mix.astype(jnp.bfloat16)
    mix_lo = (mix - mix_hi.astype(jnp.float32)).astype(jnp.bfloat16)
    mix_ref[...] = jnp.concatenate([mix_hi, mix_lo], axis=0)

    for c in range(nc):
        forward(0, c)
    for e in range(local):
        gate = jnp.zeros((n * CAP_DEV, ff), jnp.float32)
        up = jnp.zeros((n * CAP_DEV, ff), jnp.float32)
        for c in range(nc):
            cols = pl.ds(c * dc, dc)
            for copy in up_copies[e, c]:
                copy.wait()
            collect(e, c)
            x = rows_of([xr[e, c, i] for i in range(n)])
            gate += jnp.dot(x, wg[e, cols, :], preferred_element_type=jnp.float32)
            up += jnp.dot(x, wu[e, cols, :], preferred_element_type=jnp.float32)
        for c in range(nc if e + 1 < local else 0):
            forward(e + 1, c)
        hidden = (gate / (1.0 + jnp.exp(-gate)) * up).astype(jnp.bfloat16)
        for c in range(nc):
            cols = pl.ds(c * dc, dc)
            down_copies[e, c].wait()
            part = jnp.dot(hidden, wd[e, :, cols], preferred_element_type=jnp.float32)
            for i in range(n):
                ps[e, c, i] = part[i * CAP_DEV:(i + 1) * CAP_DEV].astype(jnp.bfloat16)
            for other in range(n):
                @pl.when(other != me)
                def _():
                    pltpu.make_async_remote_copy(
                        src_ref=ps.at[e, c, other],
                        dst_ref=pr.at[e, c, me],
                        send_sem=s2,
                        recv_sem=r2,
                        device_id=device(jnp.int32(other)),
                        device_id_type=MESH,
                    ).start()
            pr[e, c, me] = ps[e, c, me]
    if h < n_tp:
        @pl.when(gateway)
        def _():
            drain(xr.at[:, :, pl.ds(0, 2 * h * n_cp - 1)], s1)
            for m in range(h - 1):
                drain(xr.at[:, :, pl.ds(0, (h - 1) * n_cp)], fs.at[m])
        @pl.when(jnp.logical_not(gateway))
        def _():
            drain(xr.at[:, :, pl.ds(0, h * n_cp - 1 + n_cp)], s1)
    else:
        drain(xr.at[:, :, pl.ds(0, n - 1)], s1)
    drain(pr.at[:, :, pl.ds(0, n - 1)], s2)
    drain(pr.at[:, :, pl.ds(0, n - 1)], r2)


def combine_kernel(pr, mix_ref, out_hbm, ob, osem):
    local, nc, n, cap, dc = pr.shape
    mix = mix_ref[...]
    half = mix.shape[0] // 2
    part = dc // SPLIT
    outs = []
    for c in range(nc):
        for p in range(SPLIT):
            at = pl.ds(p * part, part)
            cols = pl.ds(c * dc + p * part, part)
            rows = rows_of([pr[e, c, i, :, at] for e in range(local) for i in range(n)])
            both = jnp.dot(mix, rows, preferred_element_type=jnp.float32)
            ob[:, cols] = (both[:half] + both[half:]).astype(jnp.bfloat16)
            copy = pltpu.make_async_copy(ob.at[:, cols], out_hbm.at[:, cols], osem.at[c, p])
            copy.start()
            outs.append(copy)
    for copy in outs:
        copy.wait()


def body(n_tp, n_cp, tokens, router, gate_weight, up_weight, down_weight, expert_ids, slot_index):
    n = n_tp * n_cp
    rows, width = tokens.shape
    local, _, ff = gate_weight.shape
    nc = CHUNKS if n <= 16 else 1
    dc = width // nc
    anywhere = pl.BlockSpec(memory_space=pl.ANY)
    resident = pl.BlockSpec(memory_space=pltpu.VMEM)
    bf16 = jnp.bfloat16
    dma = pltpu.SemaphoreType.DMA
    slab = (local, nc, n, CAP_DEV, dc)
    pr, mix = pl.pallas_call(
        functools.partial(exchange_kernel, n_tp, n_cp, nc),
        out_shape=[
            pltpu.VMEM(slab, bf16),
            pltpu.VMEM((2 * rows, local * n * CAP_DEV), bf16),
        ],
        in_specs=[anywhere] * 7,
        out_specs=[resident, resident],
        scratch_shapes=[
            pltpu.VMEM((expert_ids.shape[1], rows), jnp.int32),
            pltpu.VMEM((slot_index.shape[1], rows), jnp.int32),
            pltpu.VMEM((rows, width), bf16),
            pltpu.VMEM((router.shape[1], width), bf16),
            pltpu.VMEM((local, width, ff), bf16),
            pltpu.VMEM((local, width, ff), bf16),
            pltpu.VMEM((local, ff, width), bf16),
            pltpu.VMEM((local, nc, n_cp, CAP_DEV, dc), bf16),
            pltpu.VMEM(slab, bf16),
            pltpu.VMEM(slab, bf16),
            dma((nc + 3,)),
            dma((3, local, nc)),
            dma,
            dma((local, nc)),
            dma((max(n_tp // 2 - 1, 1),)),
            dma((local, nc, max(n_tp // 2, 1) * n_cp)),
            dma,
            dma,
        ],
        compiler_params=pltpu.CompilerParams(
            collective_id=0, has_side_effects=True, vmem_limit_bytes=60 * 1024 * 1024
        ),
    )(tokens, router.T, expert_ids.T, slot_index.T, gate_weight, up_weight, down_weight)
    return pl.pallas_call(
        combine_kernel,
        out_shape=jax.ShapeDtypeStruct((rows, width), bf16),
        in_specs=[resident, resident],
        out_specs=anywhere,
        scratch_shapes=[
            pltpu.VMEM((rows, width), bf16),
            dma((nc, SPLIT)),
        ],
        compiler_params=pltpu.CompilerParams(vmem_limit_bytes=8 * 1024 * 1024),
    )(pr, mix)


def solution(mesh):
    in_specs = (
        P(("dp", "tp", "cp"), None),
        P(),
        P("cp", None, "tp"),
        P("cp", None, "tp"),
        P("cp", "tp", None),
        P(("dp", "tp", "cp"), None),
        P(("dp", "tp", "cp"), None),
    )
    out_specs = P(("dp", "tp", "cp"), None)
    step = functools.partial(body, mesh.shape["tp"], mesh.shape["cp"])
    return jax.shard_map(step, mesh=mesh, in_specs=in_specs, out_specs=out_specs, check_vma=False)
```

```python
import functools

import jax
import jax.numpy as jnp
from jax import lax
from jax.experimental import pallas as pl
from jax.experimental.pallas import tpu as pltpu
from jax.sharding import PartitionSpec as P

CAP_DEV = 2
ROUTE_SCALE = 2.5
CHUNKS = 1
SPLIT = 4
RELAY = (1, 1)
SHARE_FIRST = False
EARLY = True
MESH = pl.DeviceIdType.MESH
NT = (((1,), (1,)), ((), ()))


def rows_of(pieces):
    return jnp.concatenate([p.astype(jnp.float32) for p in pieces], axis=0).astype(jnp.bfloat16)


def flip(index, bits):
    for b in range(bits.bit_length()):
        if (bits >> b) & 1:
            index = index + (1 - 2 * lax.rem(index // (1 << b), 2)) * (1 << b)
    return index


def exchange_kernel(
    n_tp, n_cp, nc,
    tok_hbm, rt_hbm, ids_hbm, slot_hbm, wg_hbm, wu_hbm, wd_hbm,
    pr, mix_ref,
    ids_ref, slot_ref, tok, rt, wg, wu, wd, xs, xr, ps,
    in_sem, wsem, s1, r1, fs, fr, s2, r2,
):
    n = n_tp * n_cp
    my_z, my_x = lax.axis_index("tp"), lax.axis_index("cp")
    me = my_z * n_cp + my_x
    local, width, ff = wg.shape
    dc = width // nc
    slots = n_cp * local * CAP_DEV
    pow2 = n & (n - 1) == 0
    h = n_tp // 2 if n_tp % 2 == 0 and n_tp > 2 else n_tp
    inner = (h - 1, h)
    relay = [RELAY[min(e + 2 - local, 1)] if local > 1 else 1 for e in range(local)]
    order = list(range(n - 1, 0, -1))

    def peer(j):
        return flip(me, j) if pow2 else lax.rem(me + j, n)

    def source(j):
        return flip(me, j) if pow2 else lax.rem(me + n - j, n)

    def device(other):
        return {"tp": other // n_cp, "cp": lax.rem(other, n_cp)}

    def drain(ref, sem):
        pltpu.make_async_copy(ref, ref, sem).wait()

    index_copies = [
        pltpu.make_async_copy(ids_hbm, ids_ref, in_sem.at[nc + 1]),
        pltpu.make_async_copy(slot_hbm, slot_ref, in_sem.at[nc + 2]),
    ]
    for copy in index_copies:
        copy.start()
    tok_copies = []
    for c in range(nc):
        cols = pl.ds(c * dc, dc)
        copy = pltpu.make_async_copy(tok_hbm.at[:, cols], tok.at[:, cols], in_sem.at[c])
        copy.start()
        tok_copies.append(copy)
    rt_copy = pltpu.make_async_copy(rt_hbm, rt, in_sem.at[nc])
    rt_copy.start()

    barrier = pltpu.get_barrier_semaphore()
    for j in order:
        pl.semaphore_signal(barrier, inc=1, device_id=device(peer(j)), device_id_type=MESH)

    up_copies, down_copies = {}, {}
    for e in range(local):
        for c in range(nc):
            cols = pl.ds(c * dc, dc)
            pair = [
                pltpu.make_async_copy(wg_hbm.at[e, cols, :], wg.at[e, cols, :], wsem.at[0, e, c]),
                pltpu.make_async_copy(wu_hbm.at[e, cols, :], wu.at[e, cols, :], wsem.at[1, e, c]),
            ]
            for copy in pair:
                copy.start()
            up_copies[e, c] = pair
        for c in range(nc):
            cols = pl.ds(c * dc, dc)
            copy = pltpu.make_async_copy(wd_hbm.at[e, :, cols], wd.at[e, :, cols], wsem.at[2, e, c])
            copy.start()
            down_copies[e, c] = copy

    for copy in index_copies:
        copy.wait()
    ids0, ids1 = ids_ref[0:1, :], ids_ref[1:2, :]
    slot0, slot1 = slot_ref[0:1, :], slot_ref[1:2, :]
    target0 = jnp.where(slot0 >= 0, ids0 * CAP_DEV + slot0, -1)
    target1 = jnp.where(slot1 >= 0, ids1 * CAP_DEV + slot1, -1)
    row = lax.broadcasted_iota(jnp.int32, (slots, ids0.shape[1]), 0)
    placing = jnp.where((row == target0) | (row == target1), 1.0, 0.0).astype(jnp.bfloat16)

    half = my_z // h
    gateway = (my_z == inner[0]) | (my_z == inner[-1])
    pair = range(n_tp // h)
    near = [range(b * h, b * h + h) for b in pair]

    def place(e, c, z, x, recv_sem):
        pltpu.make_async_remote_copy(
            src_ref=xs.at[e, c, x],
            dst_ref=xr.at[e, c, me],
            send_sem=s1.at[e],
            recv_sem=recv_sem,
            device_id={"tp": jnp.int32(z), "cp": jnp.int32(x)},
            device_id_type=MESH,
        ).start()

    def cross(e, c):
        for b in pair if h < n_tp else ():
            for z in sorted(near[b], key=lambda z: z != inner[b]):
                ahead = half != b
                if z != inner[b] and relay[e] == 2:
                    continue
                if z != inner[b] and relay[e] == 1:
                    ahead = ahead & gateway
                @pl.when(ahead)
                def _():
                    for x in range(n_cp):
                        place(e, c, z, x, fr.at[e, c, lax.rem(me, h * n_cp)])

    def share(e, c):
        for z in range(n_tp):
            for x in range(n_cp):
                @pl.when((half == z // h) & (me != z * n_cp + x))
                def _():
                    place(e, c, z, x, r1.at[e, c])
        xr[e, c, me] = xs[e, c, my_x]

    def sources(b, e, outer):
        mine = inner[1 - b]
        return [
            z * n_cp + x
            for z in near[1 - b] if (z != mine) == outer
            for x in range(n_cp)
        ]

    def forward(e, c, outer):
        for b in pair if h < n_tp and relay[e] > (0 if outer else 1) else ():
            @pl.when(my_z == inner[b])
            def _():
                others = [z for z in near[b] if z != inner[b]]
                for k in sources(b, e, outer):
                    drain(xr.at[e, c, k], fr.at[e, c, k % (h * n_cp)])
                    for m, z in enumerate(others):
                        pltpu.make_async_remote_copy(
                            src_ref=xr.at[e, c, k],
                            dst_ref=xr.at[e, c, k],
                            send_sem=fs.at[e, m],
                            recv_sem=fr.at[e, c, k % (h * n_cp)],
                            device_id={"tp": jnp.int32(z), "cp": my_x},
                            device_id_type=MESH,
                        ).start()

    def collect(e, c):
        if h * n_cp > 1:
            drain(xr.at[e, c, pl.ds(0, h * n_cp - 1)], r1.at[e, c])
        for b in pair if h < n_tp else ():
            for outer in (False, True):
                late = half == b
                if relay[e] > (0 if outer else 1):
                    late = late & jnp.logical_not(gateway)
                @pl.when(late)
                def _():
                    for k in sources(b, e, outer):
                        drain(xr.at[e, c, k], fr.at[e, c, k % (h * n_cp)])

    for c in range(nc):
        tok_copies[c].wait()
        cols = pl.ds(c * dc, dc)
        outgoing = jnp.dot(placing, tok[:, cols], preferred_element_type=jnp.float32)
        for x in range(n_cp):
            for e in range(local):
                at = (x * local + e) * CAP_DEV
                xs[e, c, x] = outgoing[at:at + CAP_DEV].astype(jnp.bfloat16)
        if c == 0:
            pl.semaphore_wait(barrier, n - 1)
        cross(0, c)
        if SHARE_FIRST:
            share(0, c)
    if not SHARE_FIRST:
        for c in range(nc):
            if local > 1:
                cross(1, c)
            share(0, c)
    for e in range(1, local):
        for c in range(nc):
            if SHARE_FIRST or e > 1:
                cross(e, c)
            share(e, c)

    rt_copy.wait()
    logits = lax.dot_general(rt[...], tok[...], NT, preferred_element_type=jnp.float32)
    affinity = 1.0 / (1.0 + jnp.exp(-logits))
    erow = lax.broadcasted_iota(jnp.int32, logits.shape, 0)
    chosen0 = jnp.sum(jnp.where(erow == ids0, affinity, 0.0), axis=0, keepdims=True)
    chosen1 = jnp.sum(jnp.where(erow == ids1, affinity, 0.0), axis=0, keepdims=True)
    total = chosen0 + chosen1
    share0 = ROUTE_SCALE * chosen0 / total
    share1 = ROUTE_SCALE * chosen1 / total
    wide = lax.broadcasted_iota(jnp.int32, (local * n * CAP_DEV, ids0.shape[1]), 0)
    which = lax.rem(wide // CAP_DEV, n_cp) * local + wide // (n * CAP_DEV)
    wide = which * CAP_DEV + lax.rem(wide, CAP_DEV)
    mix = jnp.where(wide == target0, share0, 0.0) + jnp.where(wide == target1, share1, 0.0)
    mix = mix.T
    mix_hi = mix.astype(jnp.bfloat16)
    mix_lo = (mix - mix_hi.astype(jnp.float32)).astype(jnp.bfloat16)
    mix_ref[...] = jnp.concatenate([mix_hi, mix_lo], axis=0)

    for e in range(local):
        for c in range(nc):
            forward(e, c, False)
            if e == 0 or EARLY:
                forward(e, c, True)
    for e in range(local):
        gate = jnp.zeros((n * CAP_DEV, ff), jnp.float32)
        up = jnp.zeros((n * CAP_DEV, ff), jnp.float32)
        for c in range(nc):
            cols = pl.ds(c * dc, dc)
            for copy in up_copies[e, c]:
                copy.wait()
            collect(e, c)
            x = rows_of([xr[e, c, i] for i in range(n)])
            gate += jnp.dot(x, wg[e, cols, :], preferred_element_type=jnp.float32)
            up += jnp.dot(x, wu[e, cols, :], preferred_element_type=jnp.float32)
        for c in range(nc if e + 1 < local and not EARLY else 0):
            forward(e + 1, c, True)
        hidden = (gate / (1.0 + jnp.exp(-gate)) * up).astype(jnp.bfloat16)
        for c in range(nc):
            cols = pl.ds(c * dc, dc)
            down_copies[e, c].wait()
            part = jnp.dot(hidden, wd[e, :, cols], preferred_element_type=jnp.float32)
            for i in range(n):
                ps[e, c, i] = part[i * CAP_DEV:(i + 1) * CAP_DEV].astype(jnp.bfloat16)
            for other in range(n):
                @pl.when(other != me)
                def _():
                    pltpu.make_async_remote_copy(
                        src_ref=ps.at[e, c, other],
                        dst_ref=pr.at[e, c, me],
                        send_sem=s2,
                        recv_sem=r2,
                        device_id=device(jnp.int32(other)),
                        device_id_type=MESH,
                    ).start()
            pr[e, c, me] = ps[e, c, me]
    for e in range(local):
        own = h * n_cp - 1
        if h == n_tp or relay[e] == 0:
            drain(xr.at[e, :, pl.ds(0, n - 1)], s1.at[e])
            continue
        @pl.when(gateway)
        def _():
            drain(xr.at[e, :, pl.ds(0, own + (h * n_cp if relay[e] == 1 else n_cp))], s1.at[e])
            for m in range(h - 1):
                drain(xr.at[e, :, pl.ds(0, (h - 2 + relay[e]) * n_cp)], fs.at[e, m])
        @pl.when(jnp.logical_not(gateway))
        def _():
            drain(xr.at[e, :, pl.ds(0, own + n_cp)], s1.at[e])
    drain(pr.at[:, :, pl.ds(0, n - 1)], s2)
    drain(pr.at[:, :, pl.ds(0, n - 1)], r2)


def combine_kernel(pr, mix_ref, out_hbm, ob, osem):
    local, nc, n, cap, dc = pr.shape
    mix = mix_ref[...]
    half = mix.shape[0] // 2
    part = dc // SPLIT
    outs = []
    for c in range(nc):
        for p in range(SPLIT):
            at = pl.ds(p * part, part)
            cols = pl.ds(c * dc + p * part, part)
            rows = rows_of([pr[e, c, i, :, at] for e in range(local) for i in range(n)])
            both = jnp.dot(mix, rows, preferred_element_type=jnp.float32)
            ob[:, cols] = (both[:half] + both[half:]).astype(jnp.bfloat16)
            copy = pltpu.make_async_copy(ob.at[:, cols], out_hbm.at[:, cols], osem.at[c, p])
            copy.start()
            outs.append(copy)
    for copy in outs:
        copy.wait()


def body(n_tp, n_cp, tokens, router, gate_weight, up_weight, down_weight, expert_ids, slot_index):
    n = n_tp * n_cp
    rows, width = tokens.shape
    local, _, ff = gate_weight.shape
    nc = CHUNKS if n <= 16 else 1
    dc = width // nc
    anywhere = pl.BlockSpec(memory_space=pl.ANY)
    resident = pl.BlockSpec(memory_space=pltpu.VMEM)
    bf16 = jnp.bfloat16
    dma = pltpu.SemaphoreType.DMA
    slab = (local, nc, n, CAP_DEV, dc)
    pr, mix = pl.pallas_call(
        functools.partial(exchange_kernel, n_tp, n_cp, nc),
        out_shape=[
            pltpu.VMEM(slab, bf16),
            pltpu.VMEM((2 * rows, local * n * CAP_DEV), bf16),
        ],
        in_specs=[anywhere] * 7,
        out_specs=[resident, resident],
        scratch_shapes=[
            pltpu.VMEM((expert_ids.shape[1], rows), jnp.int32),
            pltpu.VMEM((slot_index.shape[1], rows), jnp.int32),
            pltpu.VMEM((rows, width), bf16),
            pltpu.VMEM((router.shape[1], width), bf16),
            pltpu.VMEM((local, width, ff), bf16),
            pltpu.VMEM((local, width, ff), bf16),
            pltpu.VMEM((local, ff, width), bf16),
            pltpu.VMEM((local, nc, n_cp, CAP_DEV, dc), bf16),
            pltpu.VMEM(slab, bf16),
            pltpu.VMEM(slab, bf16),
            dma((nc + 3,)),
            dma((3, local, nc)),
            dma((local,)),
            dma((local, nc)),
            dma((local, max(n_tp // 2 - 1, 1))),
            dma((local, nc, max(n_tp // 2, 1) * n_cp)),
            dma,
            dma,
        ],
        compiler_params=pltpu.CompilerParams(
            collective_id=0, has_side_effects=True, vmem_limit_bytes=60 * 1024 * 1024
        ),
    )(tokens, router.T, expert_ids.T, slot_index.T, gate_weight, up_weight, down_weight)
    return pl.pallas_call(
        combine_kernel,
        out_shape=jax.ShapeDtypeStruct((rows, width), bf16),
        in_specs=[resident, resident],
        out_specs=anywhere,
        scratch_shapes=[
            pltpu.VMEM((rows, width), bf16),
            dma((nc, SPLIT)),
        ],
        compiler_params=pltpu.CompilerParams(vmem_limit_bytes=8 * 1024 * 1024),
    )(pr, mix)


def solution(mesh):
    in_specs = (
        P(("dp", "tp", "cp"), None),
        P(),
        P("cp", None, "tp"),
        P("cp", None, "tp"),
        P("cp", "tp", None),
        P(("dp", "tp", "cp"), None),
        P(("dp", "tp", "cp"), None),
    )
    out_specs = P(("dp", "tp", "cp"), None)
    step = functools.partial(body, mesh.shape["tp"], mesh.shape["cp"])
    return jax.shard_map(step, mesh=mesh, in_specs=in_specs, out_specs=out_specs, check_vma=False)
```

```python
import functools

import jax
import jax.numpy as jnp
from jax import lax
from jax.experimental import pallas as pl
from jax.experimental.pallas import tpu as pltpu
from jax.sharding import PartitionSpec as P

CAP_DEV = 2
ROUTE_SCALE = 2.5
CHUNKS = 1
SPLIT = 4
MERGE = lambda z, h, e: 0 < z < h and e == 0
RELAY = (1, 1)
SHARE_FIRST = False
EARLY = True
MESH = pl.DeviceIdType.MESH
NT = (((1,), (1,)), ((), ()))


def rows_of(pieces):
    return jnp.concatenate([p.astype(jnp.float32) for p in pieces], axis=0).astype(jnp.bfloat16)


def flip(index, bits):
    for b in range(bits.bit_length()):
        if (bits >> b) & 1:
            index = index + (1 - 2 * lax.rem(index // (1 << b), 2)) * (1 << b)
    return index


def exchange_kernel(
    n_tp, n_cp, nc,
    tok_hbm, rt_hbm, ids_hbm, slot_hbm, wg_hbm, wu_hbm, wd_hbm,
    pr, mix_ref,
    ids_ref, slot_ref, tok, rt, wg, wu, wd, xs, xr, ps, kept, met,
    in_sem, wsem, s1, r1, fs, fr, s2, r2, ms,
):
    n = n_tp * n_cp
    my_z, my_x = lax.axis_index("tp"), lax.axis_index("cp")
    me = my_z * n_cp + my_x
    local, width, ff = wg.shape
    dc = width // nc
    slots = n_cp * local * CAP_DEV
    pow2 = n & (n - 1) == 0
    h = n_tp // 2 if n_tp % 2 == 0 and n_tp > 2 else n_tp
    inner = (h - 1, h)
    relay = [RELAY[min(e + 2 - local, 1)] if local > 1 else 1 for e in range(local)]
    order = list(range(n - 1, 0, -1))

    def peer(j):
        return flip(me, j) if pow2 else lax.rem(me + j, n)

    def source(j):
        return flip(me, j) if pow2 else lax.rem(me + n - j, n)

    def device(other):
        return {"tp": other // n_cp, "cp": lax.rem(other, n_cp)}

    def drain(ref, sem):
        pltpu.make_async_copy(ref, ref, sem).wait()

    index_copies = [
        pltpu.make_async_copy(ids_hbm, ids_ref, in_sem.at[nc + 1]),
        pltpu.make_async_copy(slot_hbm, slot_ref, in_sem.at[nc + 2]),
    ]
    for copy in index_copies:
        copy.start()
    tok_copies = []
    for c in range(nc):
        cols = pl.ds(c * dc, dc)
        copy = pltpu.make_async_copy(tok_hbm.at[:, cols], tok.at[:, cols], in_sem.at[c])
        copy.start()
        tok_copies.append(copy)
    rt_copy = pltpu.make_async_copy(rt_hbm, rt, in_sem.at[nc])
    rt_copy.start()

    barrier = pltpu.get_barrier_semaphore()
    for j in order:
        pl.semaphore_signal(barrier, inc=1, device_id=device(peer(j)), device_id_type=MESH)

    up_copies, down_copies = {}, {}
    for e in range(local):
        for c in range(nc):
            cols = pl.ds(c * dc, dc)
            pair = [
                pltpu.make_async_copy(wg_hbm.at[e, cols, :], wg.at[e, cols, :], wsem.at[0, e, c]),
                pltpu.make_async_copy(wu_hbm.at[e, cols, :], wu.at[e, cols, :], wsem.at[1, e, c]),
            ]
            for copy in pair:
                copy.start()
            up_copies[e, c] = pair
        for c in range(nc):
            cols = pl.ds(c * dc, dc)
            copy = pltpu.make_async_copy(wd_hbm.at[e, :, cols], wd.at[e, :, cols], wsem.at[2, e, c])
            copy.start()
            down_copies[e, c] = copy

    for copy in index_copies:
        copy.wait()
    ids0, ids1 = ids_ref[0:1, :], ids_ref[1:2, :]
    slot0, slot1 = slot_ref[0:1, :], slot_ref[1:2, :]
    target0 = jnp.where(slot0 >= 0, ids0 * CAP_DEV + slot0, -1)
    target1 = jnp.where(slot1 >= 0, ids1 * CAP_DEV + slot1, -1)
    row = lax.broadcasted_iota(jnp.int32, (slots, ids0.shape[1]), 0)
    placing = jnp.where((row == target0) | (row == target1), 1.0, 0.0).astype(jnp.bfloat16)

    half = my_z // h
    gateway = (my_z == inner[0]) | (my_z == inner[-1])
    pair = range(n_tp // h)
    near = [range(b * h, b * h + h) for b in pair]

    def place(e, c, z, x, recv_sem):
        pltpu.make_async_remote_copy(
            src_ref=xs.at[e, c, x],
            dst_ref=xr.at[e, c, me],
            send_sem=s1.at[e],
            recv_sem=recv_sem,
            device_id={"tp": jnp.int32(z), "cp": jnp.int32(x)},
            device_id_type=MESH,
        ).start()

    def cross(e, c):
        for b in pair if h < n_tp else ():
            for z in sorted(near[b], key=lambda z: z != inner[b]):
                ahead = half != b
                if z != inner[b] and relay[e] == 2:
                    continue
                if z != inner[b] and relay[e] == 1:
                    ahead = ahead & gateway
                @pl.when(ahead)
                def _():
                    for x in range(n_cp):
                        place(e, c, z, x, fr.at[e, c, lax.rem(me, h * n_cp)])

    def share(e, c):
        for z in range(n_tp):
            for x in range(n_cp):
                @pl.when((half == z // h) & (me != z * n_cp + x))
                def _():
                    place(e, c, z, x, r1.at[e, c])
        xr[e, c, me] = xs[e, c, my_x]

    def sources(b, e, outer):
        mine = inner[1 - b]
        return [
            z * n_cp + x
            for z in near[1 - b] if (z != mine) == outer
            for x in range(n_cp)
        ]

    def forward(e, c, outer):
        for b in pair if h < n_tp and relay[e] > (0 if outer else 1) else ():
            @pl.when(my_z == inner[b])
            def _():
                others = [z for z in near[b] if z != inner[b]]
                for k in sources(b, e, outer):
                    drain(xr.at[e, c, k], fr.at[e, c, k % (h * n_cp)])
                    for m, z in enumerate(others):
                        pltpu.make_async_remote_copy(
                            src_ref=xr.at[e, c, k],
                            dst_ref=xr.at[e, c, k],
                            send_sem=fs.at[e, m],
                            recv_sem=fr.at[e, c, k % (h * n_cp)],
                            device_id={"tp": jnp.int32(z), "cp": my_x},
                            device_id_type=MESH,
                        ).start()

    def collect(e, c):
        if h * n_cp > 1:
            drain(xr.at[e, c, pl.ds(0, h * n_cp - 1)], r1.at[e, c])
        for b in pair if h < n_tp else ():
            for outer in (False, True):
                late = half == b
                if relay[e] > (0 if outer else 1):
                    late = late & jnp.logical_not(gateway)
                @pl.when(late)
                def _():
                    for k in sources(b, e, outer):
                        drain(xr.at[e, c, k], fr.at[e, c, k % (h * n_cp)])

    for c in range(nc):
        tok_copies[c].wait()
        cols = pl.ds(c * dc, dc)
        outgoing = jnp.dot(placing, tok[:, cols], preferred_element_type=jnp.float32)
        for x in range(n_cp):
            for e in range(local):
                at = (x * local + e) * CAP_DEV
                xs[e, c, x] = outgoing[at:at + CAP_DEV].astype(jnp.bfloat16)
        if c == 0:
            pl.semaphore_wait(barrier, n - 1)
        cross(0, c)
        if SHARE_FIRST:
            share(0, c)
    if not SHARE_FIRST:
        for c in range(nc):
            if local > 1:
                cross(1, c)
            share(0, c)
    for e in range(1, local):
        for c in range(nc):
            if SHARE_FIRST or e > 1:
                cross(e, c)
            share(e, c)

    rt_copy.wait()
    logits = lax.dot_general(rt[...], tok[...], NT, preferred_element_type=jnp.float32)
    affinity = 1.0 / (1.0 + jnp.exp(-logits))
    erow = lax.broadcasted_iota(jnp.int32, logits.shape, 0)
    chosen0 = jnp.sum(jnp.where(erow == ids0, affinity, 0.0), axis=0, keepdims=True)
    chosen1 = jnp.sum(jnp.where(erow == ids1, affinity, 0.0), axis=0, keepdims=True)
    total = chosen0 + chosen1
    share0 = ROUTE_SCALE * chosen0 / total
    share1 = ROUTE_SCALE * chosen1 / total
    wide = lax.broadcasted_iota(jnp.int32, (local * n * CAP_DEV, ids0.shape[1]), 0)
    which = lax.rem(wide // CAP_DEV, n_cp) * local + wide // (n * CAP_DEV)
    wide = which * CAP_DEV + lax.rem(wide, CAP_DEV)
    mix = jnp.where(wide == target0, share0, 0.0) + jnp.where(wide == target1, share1, 0.0)
    mix = mix.T
    mix_hi = mix.astype(jnp.bfloat16)
    mix_lo = (mix - mix_hi.astype(jnp.float32)).astype(jnp.bfloat16)
    mix_ref[...] = jnp.concatenate([mix_hi, mix_lo], axis=1)

    for e in range(local):
        for c in range(nc):
            forward(e, c, False)
            if e == 0 or EARLY:
                forward(e, c, True)
    rank = jnp.where(half == 0, my_z, my_z - h - 1)

    def merged(z, e):
        return h < n_tp and MERGE(z, h, e)

    def give_back(e, c, other):
        pltpu.make_async_remote_copy(
            src_ref=ps.at[e, c, other],
            dst_ref=pr.at[e, c, me],
            send_sem=s2,
            recv_sem=r2.at[e],
            device_id=device(jnp.int32(other)),
            device_id_type=MESH,
        ).start()

    for z in range(n_tp):
        for e in range(local):
            if merged(z, e):
                @pl.when(my_z == z)
                def _():
                    for k in sources(z // h, e, True):
                        for c in range(nc):
                            pr[e, c, k] = jnp.zeros(pr.shape[3:], pr.dtype)

    for e in range(local):
        gate = jnp.zeros((n * CAP_DEV, ff), jnp.float32)
        up = jnp.zeros((n * CAP_DEV, ff), jnp.float32)
        for c in range(nc):
            cols = pl.ds(c * dc, dc)
            for copy in up_copies[e, c]:
                copy.wait()
            collect(e, c)
            x = rows_of([xr[e, c, i] for i in range(n)])
            gate += jnp.dot(x, wg[e, cols, :], preferred_element_type=jnp.float32)
            up += jnp.dot(x, wu[e, cols, :], preferred_element_type=jnp.float32)
        for c in range(nc if e + 1 < local and not EARLY else 0):
            forward(e + 1, c, True)
        hidden = (gate / (1.0 + jnp.exp(-gate)) * up).astype(jnp.bfloat16)
        for c in range(nc):
            cols = pl.ds(c * dc, dc)
            down_copies[e, c].wait()
            part = jnp.dot(hidden, wd[e, :, cols], preferred_element_type=jnp.float32)
            for other in range(n):
                z = other // n_cp
                ps[e, c, other] = part[other * CAP_DEV:(other + 1) * CAP_DEV].astype(jnp.bfloat16)
                aside = z // h != half
                direct = other != me
                if merged(z, e):
                    direct = direct & jnp.logical_not(aside)
                @pl.when(direct)
                def _():
                    give_back(e, c, other)
                if merged(z, e):
                    at = other % (h * n_cp)
                    @pl.when(aside & gateway)
                    def _():
                        kept[e, c, at] = part[other * CAP_DEV:(other + 1) * CAP_DEV]
                    for b in pair:
                        if z // h == b:
                            continue
                        @pl.when((half == b) & jnp.logical_not(gateway))
                        def _():
                            pltpu.make_async_remote_copy(
                                src_ref=ps.at[e, c, other],
                                dst_ref=met.at[e, c, at, rank],
                                send_sem=s2,
                                recv_sem=ms.at[e],
                                device_id={"tp": jnp.int32(inner[b]), "cp": my_x},
                                device_id_type=MESH,
                            ).start()
            pr[e, c, me] = ps[e, c, me]
    for e in range(local):
        for b in pair if h < n_tp else ():
            ends = [z * n_cp + x for z in near[1 - b] if merged(z, e) for x in range(n_cp)]
            if not ends:
                continue
            @pl.when(my_z == inner[b])
            def _():
                drain(met.at[e, :, pl.ds(0, len(ends))], ms.at[e])
                for c in range(nc):
                    for other in ends:
                        at = other % (h * n_cp)
                        total = kept[e, c, at]
                        for m in range(h - 1):
                            total = total + met[e, c, at, m].astype(jnp.float32)
                        ps[e, c, other] = total.astype(jnp.bfloat16)
                        give_back(e, c, other)
    for e in range(local):
        own = h * n_cp - 1
        if h == n_tp or relay[e] == 0:
            drain(xr.at[e, :, pl.ds(0, n - 1)], s1.at[e])
            continue
        @pl.when(gateway)
        def _():
            drain(xr.at[e, :, pl.ds(0, own + (h * n_cp if relay[e] == 1 else n_cp))], s1.at[e])
            for m in range(h - 1):
                drain(xr.at[e, :, pl.ds(0, (h - 2 + relay[e]) * n_cp)], fs.at[e, m])
        @pl.when(jnp.logical_not(gateway))
        def _():
            drain(xr.at[e, :, pl.ds(0, own + n_cp)], s1.at[e])
    drain(pr.at[:, :, pl.ds(0, n - 1)], s2)
    for e in range(local):
        counts = [h * n_cp - 1 + n_cp if merged(z, e) else n - 1 for z in range(n_tp)]
        for count in sorted(set(counts)):
            here = [z for z in range(n_tp) if counts[z] == count]
            if len(here) == n_tp:
                drain(pr.at[e, :, pl.ds(0, count)], r2.at[e])
                continue
            @pl.when(functools.reduce(jnp.logical_or, [my_z == z for z in here]))
            def _():
                drain(pr.at[e, :, pl.ds(0, count)], r2.at[e])


def combine_kernel(pr, mix_ref, out_hbm, ob, osem):
    local, nc, n, cap, dc = pr.shape
    mix = mix_ref[...]
    part = dc // SPLIT
    outs = []
    for c in range(nc):
        for p in range(SPLIT):
            at = pl.ds(p * part, part)
            cols = pl.ds(c * dc + p * part, part)
            rows = rows_of([pr[e, c, i, :, at] for e in range(local) for i in range(n)])
            rows = jnp.concatenate([rows, rows], axis=0)
            ob[:, cols] = jnp.dot(mix, rows, preferred_element_type=jnp.float32).astype(jnp.bfloat16)
            copy = pltpu.make_async_copy(ob.at[:, cols], out_hbm.at[:, cols], osem.at[c, p])
            copy.start()
            outs.append(copy)
    for copy in outs:
        copy.wait()


def body(n_tp, n_cp, tokens, router, gate_weight, up_weight, down_weight, expert_ids, slot_index):
    n = n_tp * n_cp
    rows, width = tokens.shape
    local, _, ff = gate_weight.shape
    nc = CHUNKS if n <= 16 else 1
    dc = width // nc
    anywhere = pl.BlockSpec(memory_space=pl.ANY)
    resident = pl.BlockSpec(memory_space=pltpu.VMEM)
    bf16 = jnp.bfloat16
    dma = pltpu.SemaphoreType.DMA
    slab = (local, nc, n, CAP_DEV, dc)
    across = max(n_tp // 2, 1) * n_cp
    pr, mix = pl.pallas_call(
        functools.partial(exchange_kernel, n_tp, n_cp, nc),
        out_shape=[
            pltpu.VMEM(slab, bf16),
            pltpu.VMEM((rows, 2 * local * n * CAP_DEV), bf16),
        ],
        in_specs=[anywhere] * 7,
        out_specs=[resident, resident],
        scratch_shapes=[
            pltpu.VMEM((expert_ids.shape[1], rows), jnp.int32),
            pltpu.VMEM((slot_index.shape[1], rows), jnp.int32),
            pltpu.VMEM((rows, width), bf16),
            pltpu.VMEM((router.shape[1], width), bf16),
            pltpu.VMEM((local, width, ff), bf16),
            pltpu.VMEM((local, width, ff), bf16),
            pltpu.VMEM((local, ff, width), bf16),
            pltpu.VMEM((local, nc, n_cp, CAP_DEV, dc), bf16),
            pltpu.VMEM(slab, bf16),
            pltpu.VMEM(slab, bf16),
            pltpu.VMEM((local, nc, across, CAP_DEV, dc), jnp.float32),
            pltpu.VMEM((local, nc, across, max(n_tp // 2 - 1, 1), CAP_DEV, dc), bf16),
            dma((nc + 3,)),
            dma((3, local, nc)),
            dma((local,)),
            dma((local, nc)),
            dma((local, max(n_tp // 2 - 1, 1))),
            dma((local, nc, across)),
            dma,
            dma((local,)),
            dma((local,)),
        ],
        compiler_params=pltpu.CompilerParams(
            collective_id=0, has_side_effects=True, vmem_limit_bytes=60 * 1024 * 1024
        ),
    )(tokens, router.T, expert_ids.T, slot_index.T, gate_weight, up_weight, down_weight)
    return pl.pallas_call(
        combine_kernel,
        out_shape=jax.ShapeDtypeStruct((rows, width), bf16),
        in_specs=[resident, resident],
        out_specs=anywhere,
        scratch_shapes=[
            pltpu.VMEM((rows, width), bf16),
            dma((nc, SPLIT)),
        ],
        compiler_params=pltpu.CompilerParams(vmem_limit_bytes=8 * 1024 * 1024),
    )(pr, mix)


def solution(mesh):
    in_specs = (
        P(("dp", "tp", "cp"), None),
        P(),
        P("cp", None, "tp"),
        P("cp", None, "tp"),
        P("cp", "tp", None),
        P(("dp", "tp", "cp"), None),
        P(("dp", "tp", "cp"), None),
    )
    out_specs = P(("dp", "tp", "cp"), None)
    step = functools.partial(body, mesh.shape["tp"], mesh.shape["cp"])
    return jax.shard_map(step, mesh=mesh, in_specs=in_specs, out_specs=out_specs, check_vma=False)
```

```python
import functools

import jax
import jax.numpy as jnp
from jax import lax
from jax.experimental import pallas as pl
from jax.experimental.pallas import tpu as pltpu
from jax.sharding import PartitionSpec as P

CAP_DEV = 2
ROUTE_SCALE = 2.5
CHUNKS = 1
SPLIT = 4
MERGE = lambda z, h, e: 0 < z < h and e == 0
RELAY = (1, 1)
SHARE_FIRST = False
EARLY = True
MESH = pl.DeviceIdType.MESH
NT = (((1,), (1,)), ((), ()))


def rows_of(pieces):
    return jnp.concatenate([p.astype(jnp.float32) for p in pieces], axis=0).astype(jnp.bfloat16)


def flip(index, bits):
    for b in range(bits.bit_length()):
        if (bits >> b) & 1:
            index = index + (1 - 2 * lax.rem(index // (1 << b), 2)) * (1 << b)
    return index


def exchange_kernel(
    n_tp, n_cp, nc,
    tok_hbm, rt_hbm, ids_hbm, slot_hbm, wg_hbm, wu_hbm, wd_hbm,
    pr, mix_ref,
    ids_ref, slot_ref, tok, rt, wg, wu, wd, xs, xr, ps, kept, met,
    in_sem, wsem, s1, r1, fs, fr, s2, r2, ms,
):
    n = n_tp * n_cp
    my_z, my_x = lax.axis_index("tp"), lax.axis_index("cp")
    me = my_z * n_cp + my_x
    local, width, ff = wg.shape
    dc = width // nc
    slots = n_cp * local * CAP_DEV
    pow2 = n & (n - 1) == 0
    h = n_tp // 2 if n_tp % 2 == 0 and n_tp > 2 else n_tp
    inner = (h - 1, h)
    relay = [RELAY[min(e + 2 - local, 1)] if local > 1 else 1 for e in range(local)]
    order = list(range(n - 1, 0, -1))

    def peer(j):
        return flip(me, j) if pow2 else lax.rem(me + j, n)

    def source(j):
        return flip(me, j) if pow2 else lax.rem(me + n - j, n)

    def device(other):
        return {"tp": other // n_cp, "cp": lax.rem(other, n_cp)}

    def drain(ref, sem):
        pltpu.make_async_copy(ref, ref, sem).wait()

    index_copies = [
        pltpu.make_async_copy(ids_hbm, ids_ref, in_sem.at[nc + 1]),
        pltpu.make_async_copy(slot_hbm, slot_ref, in_sem.at[nc + 2]),
    ]
    for copy in index_copies:
        copy.start()
    tok_copies = []
    for c in range(nc):
        cols = pl.ds(c * dc, dc)
        copy = pltpu.make_async_copy(tok_hbm.at[:, cols], tok.at[:, cols], in_sem.at[c])
        copy.start()
        tok_copies.append(copy)
    rt_copy = pltpu.make_async_copy(rt_hbm, rt, in_sem.at[nc])
    rt_copy.start()

    barrier = pltpu.get_barrier_semaphore()
    for j in order:
        pl.semaphore_signal(barrier, inc=1, device_id=device(peer(j)), device_id_type=MESH)

    up_copies, down_copies = {}, {}
    for e in range(local):
        for c in range(nc):
            cols = pl.ds(c * dc, dc)
            pair = [
                pltpu.make_async_copy(wg_hbm.at[e, cols, :], wg.at[e, cols, :], wsem.at[0, e, c]),
                pltpu.make_async_copy(wu_hbm.at[e, cols, :], wu.at[e, cols, :], wsem.at[1, e, c]),
            ]
            for copy in pair:
                copy.start()
            up_copies[e, c] = pair
        for c in range(nc):
            cols = pl.ds(c * dc, dc)
            copy = pltpu.make_async_copy(wd_hbm.at[e, :, cols], wd.at[e, :, cols], wsem.at[2, e, c])
            copy.start()
            down_copies[e, c] = copy

    for copy in index_copies:
        copy.wait()
    ids0, ids1 = ids_ref[0:1, :], ids_ref[1:2, :]
    slot0, slot1 = slot_ref[0:1, :], slot_ref[1:2, :]
    target0 = jnp.where(slot0 >= 0, ids0 * CAP_DEV + slot0, -1)
    target1 = jnp.where(slot1 >= 0, ids1 * CAP_DEV + slot1, -1)
    row = lax.broadcasted_iota(jnp.int32, (slots, ids0.shape[1]), 0)
    placing = jnp.where((row == target0) | (row == target1), 1.0, 0.0).astype(jnp.bfloat16)

    half = my_z // h
    gateway = (my_z == inner[0]) | (my_z == inner[-1])
    pair = range(n_tp // h)
    near = [range(b * h, b * h + h) for b in pair]

    def place(e, c, z, x, recv_sem):
        pltpu.make_async_remote_copy(
            src_ref=xs.at[e, c, x],
            dst_ref=xr.at[e, c, me],
            send_sem=s1.at[e],
            recv_sem=recv_sem,
            device_id={"tp": jnp.int32(z), "cp": jnp.int32(x)},
            device_id_type=MESH,
        ).start()

    def cross(e, c):
        for b in pair if h < n_tp else ():
            for z in sorted(near[b], key=lambda z: z != inner[b]):
                ahead = half != b
                if z != inner[b] and relay[e] == 2:
                    continue
                if z != inner[b] and relay[e] == 1:
                    ahead = ahead & gateway
                @pl.when(ahead)
                def _():
                    for x in [lax.rem(my_x + i, n_cp) for i in range(1, n_cp + 1)]:
                        place(e, c, z, x, fr.at[e, c, lax.rem(me, h * n_cp)])

    def share(e, c):
        for z in range(n_tp):
            for x in range(n_cp):
                @pl.when((half == z // h) & (me != z * n_cp + x))
                def _():
                    place(e, c, z, x, r1.at[e, c])
        xr[e, c, me] = xs[e, c, my_x]

    def sources(b, e, outer):
        mine = inner[1 - b]
        return [
            z * n_cp + x
            for z in near[1 - b] if (z != mine) == outer
            for x in range(n_cp)
        ]

    def forward(e, c, outer):
        for b in pair if h < n_tp and relay[e] > (0 if outer else 1) else ():
            @pl.when(my_z == inner[b])
            def _():
                others = [z for z in near[b] if z != inner[b]]
                for k in sources(b, e, outer):
                    drain(xr.at[e, c, k], fr.at[e, c, k % (h * n_cp)])
                    for m, z in enumerate(others):
                        pltpu.make_async_remote_copy(
                            src_ref=xr.at[e, c, k],
                            dst_ref=xr.at[e, c, k],
                            send_sem=fs.at[e, m],
                            recv_sem=fr.at[e, c, k % (h * n_cp)],
                            device_id={"tp": jnp.int32(z), "cp": my_x},
                            device_id_type=MESH,
                        ).start()

    def collect(e, c):
        if h * n_cp > 1:
            drain(xr.at[e, c, pl.ds(0, h * n_cp - 1)], r1.at[e, c])
        for b in pair if h < n_tp else ():
            for outer in (False, True):
                late = half == b
                if relay[e] > (0 if outer else 1):
                    late = late & jnp.logical_not(gateway)
                @pl.when(late)
                def _():
                    for k in sources(b, e, outer):
                        drain(xr.at[e, c, k], fr.at[e, c, k % (h * n_cp)])

    for c in range(nc):
        tok_copies[c].wait()
        cols = pl.ds(c * dc, dc)
        outgoing = jnp.dot(placing, tok[:, cols], preferred_element_type=jnp.float32)
        for x in range(n_cp):
            for e in range(local):
                at = (x * local + e) * CAP_DEV
                xs[e, c, x] = outgoing[at:at + CAP_DEV].astype(jnp.bfloat16)
        if c == 0:
            pl.semaphore_wait(barrier, n - 1)
        if c == nc - 1:
            @pl.when(gateway)
            def _():
                for e in range(local):
                    for k in range(nc):
                        share(e, k)
                        cross(e, k)
            @pl.when(jnp.logical_not(gateway))
            def _():
                for step in (cross, share):
                    for e in range(local):
                        for k in range(nc):
                            step(e, k)

    rt_copy.wait()
    logits = lax.dot_general(rt[...], tok[...], NT, preferred_element_type=jnp.float32)
    affinity = 1.0 / (1.0 + jnp.exp(-logits))
    erow = lax.broadcasted_iota(jnp.int32, logits.shape, 0)
    chosen0 = jnp.sum(jnp.where(erow == ids0, affinity, 0.0), axis=0, keepdims=True)
    chosen1 = jnp.sum(jnp.where(erow == ids1, affinity, 0.0), axis=0, keepdims=True)
    total = chosen0 + chosen1
    share0 = ROUTE_SCALE * chosen0 / total
    share1 = ROUTE_SCALE * chosen1 / total
    wide = lax.broadcasted_iota(jnp.int32, (local * n * CAP_DEV, ids0.shape[1]), 0)
    which = lax.rem(wide // CAP_DEV, n_cp) * local + wide // (n * CAP_DEV)
    wide = which * CAP_DEV + lax.rem(wide, CAP_DEV)
    mix = jnp.where(wide == target0, share0, 0.0) + jnp.where(wide == target1, share1, 0.0)
    mix = mix.T
    mix_hi = mix.astype(jnp.bfloat16)
    mix_lo = (mix - mix_hi.astype(jnp.float32)).astype(jnp.bfloat16)
    mix_ref[...] = jnp.concatenate([mix_hi, mix_lo], axis=1)

    for e in range(local):
        for c in range(nc):
            forward(e, c, False)
            if e == 0 or EARLY:
                forward(e, c, True)
    rank = jnp.where(half == 0, my_z, my_z - h - 1)

    def merged(z, e):
        return h < n_tp and MERGE(z, h, e)

    def give_back(e, c, other):
        pltpu.make_async_remote_copy(
            src_ref=ps.at[e, c, other],
            dst_ref=pr.at[e, c, me],
            send_sem=s2,
            recv_sem=r2.at[e],
            device_id=device(jnp.int32(other)),
            device_id_type=MESH,
        ).start()

    for z in range(n_tp):
        for e in range(local):
            if merged(z, e):
                @pl.when(my_z == z)
                def _():
                    for k in sources(z // h, e, True):
                        for c in range(nc):
                            pr[e, c, k] = jnp.zeros(pr.shape[3:], pr.dtype)

    for e in range(local):
        gate = jnp.zeros((n * CAP_DEV, ff), jnp.float32)
        up = jnp.zeros((n * CAP_DEV, ff), jnp.float32)
        for c in range(nc):
            cols = pl.ds(c * dc, dc)
            for copy in up_copies[e, c]:
                copy.wait()
            collect(e, c)
            x = rows_of([xr[e, c, i] for i in range(n)])
            gate += jnp.dot(x, wg[e, cols, :], preferred_element_type=jnp.float32)
            up += jnp.dot(x, wu[e, cols, :], preferred_element_type=jnp.float32)
        for c in range(nc if e + 1 < local and not EARLY else 0):
            forward(e + 1, c, True)
        hidden = (gate / (1.0 + jnp.exp(-gate)) * up).astype(jnp.bfloat16)
        for c in range(nc):
            cols = pl.ds(c * dc, dc)
            down_copies[e, c].wait()
            part = jnp.dot(hidden, wd[e, :, cols], preferred_element_type=jnp.float32)
            turns = [z * n_cp + x for z in range(n_tp) for x in (reversed(range(n_cp)) if e < local - 1 else range(n_cp))]
            for other in turns:
                z = other // n_cp
                ps[e, c, other] = part[other * CAP_DEV:(other + 1) * CAP_DEV].astype(jnp.bfloat16)
                aside = z // h != half
                direct = other != me
                if merged(z, e):
                    direct = direct & jnp.logical_not(aside)
                @pl.when(direct)
                def _():
                    give_back(e, c, other)
                if merged(z, e):
                    at = other % (h * n_cp)
                    @pl.when(aside & gateway)
                    def _():
                        kept[e, c, at] = part[other * CAP_DEV:(other + 1) * CAP_DEV]
                    for b in pair:
                        if z // h == b:
                            continue
                        @pl.when((half == b) & jnp.logical_not(gateway))
                        def _():
                            pltpu.make_async_remote_copy(
                                src_ref=ps.at[e, c, other],
                                dst_ref=met.at[e, c, at, rank],
                                send_sem=s2,
                                recv_sem=ms.at[e],
                                device_id={"tp": jnp.int32(inner[b]), "cp": my_x},
                                device_id_type=MESH,
                            ).start()
            pr[e, c, me] = ps[e, c, me]
    for e in range(local):
        for b in pair if h < n_tp else ():
            ends = [z * n_cp + x for z in near[1 - b] if merged(z, e) for x in range(n_cp)]
            if not ends:
                continue
            @pl.when(my_z == inner[b])
            def _():
                drain(met.at[e, :, pl.ds(0, len(ends))], ms.at[e])
                for c in range(nc):
                    for other in ends:
                        at = other % (h * n_cp)
                        total = kept[e, c, at]
                        for m in range(h - 1):
                            total = total + met[e, c, at, m].astype(jnp.float32)
                        ps[e, c, other] = total.astype(jnp.bfloat16)
                        give_back(e, c, other)
    for e in range(local):
        own = h * n_cp - 1
        if h == n_tp or relay[e] == 0:
            drain(xr.at[e, :, pl.ds(0, n - 1)], s1.at[e])
            continue
        @pl.when(gateway)
        def _():
            drain(xr.at[e, :, pl.ds(0, own + (h * n_cp if relay[e] == 1 else n_cp))], s1.at[e])
            for m in range(h - 1):
                drain(xr.at[e, :, pl.ds(0, (h - 2 + relay[e]) * n_cp)], fs.at[e, m])
        @pl.when(jnp.logical_not(gateway))
        def _():
            drain(xr.at[e, :, pl.ds(0, own + n_cp)], s1.at[e])
    drain(pr.at[:, :, pl.ds(0, n - 1)], s2)
    for e in range(local):
        counts = [h * n_cp - 1 + n_cp if merged(z, e) else n - 1 for z in range(n_tp)]
        for count in sorted(set(counts)):
            here = [z for z in range(n_tp) if counts[z] == count]
            if len(here) == n_tp:
                drain(pr.at[e, :, pl.ds(0, count)], r2.at[e])
                continue
            @pl.when(functools.reduce(jnp.logical_or, [my_z == z for z in here]))
            def _():
                drain(pr.at[e, :, pl.ds(0, count)], r2.at[e])


def combine_kernel(pr, mix_ref, out_hbm, ob, osem):
    local, nc, n, cap, dc = pr.shape
    mix = mix_ref[...]
    part = dc // SPLIT
    outs = []
    for c in range(nc):
        for p in range(SPLIT):
            at = pl.ds(p * part, part)
            cols = pl.ds(c * dc + p * part, part)
            rows = rows_of([pr[e, c, i, :, at] for e in range(local) for i in range(n)])
            rows = jnp.concatenate([rows, rows], axis=0)
            ob[:, cols] = jnp.dot(mix, rows, preferred_element_type=jnp.float32).astype(jnp.bfloat16)
            copy = pltpu.make_async_copy(ob.at[:, cols], out_hbm.at[:, cols], osem.at[c, p])
            copy.start()
            outs.append(copy)
    for copy in outs:
        copy.wait()


def body(n_tp, n_cp, tokens, router, gate_weight, up_weight, down_weight, expert_ids, slot_index):
    n = n_tp * n_cp
    rows, width = tokens.shape
    local, _, ff = gate_weight.shape
    nc = CHUNKS if n <= 16 else 1
    dc = width // nc
    anywhere = pl.BlockSpec(memory_space=pl.ANY)
    resident = pl.BlockSpec(memory_space=pltpu.VMEM)
    bf16 = jnp.bfloat16
    dma = pltpu.SemaphoreType.DMA
    slab = (local, nc, n, CAP_DEV, dc)
    across = max(n_tp // 2, 1) * n_cp
    pr, mix = pl.pallas_call(
        functools.partial(exchange_kernel, n_tp, n_cp, nc),
        out_shape=[
            pltpu.VMEM(slab, bf16),
            pltpu.VMEM((rows, 2 * local * n * CAP_DEV), bf16),
        ],
        in_specs=[anywhere] * 7,
        out_specs=[resident, resident],
        scratch_shapes=[
            pltpu.VMEM((expert_ids.shape[1], rows), jnp.int32),
            pltpu.VMEM((slot_index.shape[1], rows), jnp.int32),
            pltpu.VMEM((rows, width), bf16),
            pltpu.VMEM((router.shape[1], width), bf16),
            pltpu.VMEM((local, width, ff), bf16),
            pltpu.VMEM((local, width, ff), bf16),
            pltpu.VMEM((local, ff, width), bf16),
            pltpu.VMEM((local, nc, n_cp, CAP_DEV, dc), bf16),
            pltpu.VMEM(slab, bf16),
            pltpu.VMEM(slab, bf16),
            pltpu.VMEM((local, nc, across, CAP_DEV, dc), jnp.float32),
            pltpu.VMEM((local, nc, across, max(n_tp // 2 - 1, 1), CAP_DEV, dc), bf16),
            dma((nc + 3,)),
            dma((3, local, nc)),
            dma((local,)),
            dma((local, nc)),
            dma((local, max(n_tp // 2 - 1, 1))),
            dma((local, nc, across)),
            dma,
            dma((local,)),
            dma((local,)),
        ],
        compiler_params=pltpu.CompilerParams(
            collective_id=0, has_side_effects=True, vmem_limit_bytes=60 * 1024 * 1024
        ),
    )(tokens, router.T, expert_ids.T, slot_index.T, gate_weight, up_weight, down_weight)
    return pl.pallas_call(
        combine_kernel,
        out_shape=jax.ShapeDtypeStruct((rows, width), bf16),
        in_specs=[resident, resident],
        out_specs=anywhere,
        scratch_shapes=[
            pltpu.VMEM((rows, width), bf16),
            dma((nc, SPLIT)),
        ],
        compiler_params=pltpu.CompilerParams(vmem_limit_bytes=8 * 1024 * 1024),
    )(pr, mix)


def solution(mesh):
    in_specs = (
        P(("dp", "tp", "cp"), None),
        P(),
        P("cp", None, "tp"),
        P("cp", None, "tp"),
        P("cp", "tp", None),
        P(("dp", "tp", "cp"), None),
        P(("dp", "tp", "cp"), None),
    )
    out_specs = P(("dp", "tp", "cp"), None)
    step = functools.partial(body, mesh.shape["tp"], mesh.shape["cp"])
    return jax.shard_map(step, mesh=mesh, in_specs=in_specs, out_specs=out_specs, check_vma=False)
```

```python
import functools

import jax
import jax.numpy as jnp
from jax import lax
from jax.experimental import pallas as pl
from jax.experimental.pallas import tpu as pltpu
from jax.sharding import PartitionSpec as P

CAP_DEV = 2
ROUTE_SCALE = 2.5
CHUNKS = 1
SPLIT = 4
MERGE = lambda z, h, e: 0 < z < h and e == 0
RELAY = (1, 1)
SHARE_FIRST = False
EARLY = True
MESH = pl.DeviceIdType.MESH
NT = (((1,), (1,)), ((), ()))


def rows_of(pieces):
    return jnp.concatenate([p.astype(jnp.float32) for p in pieces], axis=0).astype(jnp.bfloat16)


def flip(index, bits):
    for b in range(bits.bit_length()):
        if (bits >> b) & 1:
            index = index + (1 - 2 * lax.rem(index // (1 << b), 2)) * (1 << b)
    return index


def exchange_kernel(
    n_tp, n_cp, nc,
    tok_hbm, rt_hbm, ids_hbm, slot_hbm, wg_hbm, wu_hbm, wd_hbm,
    pr, mix_ref, base,
    ids_ref, slot_ref, tok, rt, wg, wu, wd, xs, xr, ps, kept, met,
    in_sem, wsem, s1, r1, fs, fr, s2, r2, ms,
):
    n = n_tp * n_cp
    my_z, my_x = lax.axis_index("tp"), lax.axis_index("cp")
    me = my_z * n_cp + my_x
    local, width, ff = wg.shape
    dc = width // nc
    slots = n_cp * local * CAP_DEV
    pow2 = n & (n - 1) == 0
    h = n_tp // 2 if n_tp % 2 == 0 and n_tp > 2 else n_tp
    inner = (h - 1, h)
    relay = [RELAY[min(e + 2 - local, 1)] if local > 1 else 1 for e in range(local)]
    order = list(range(n - 1, 0, -1))

    def peer(j):
        return flip(me, j) if pow2 else lax.rem(me + j, n)

    def source(j):
        return flip(me, j) if pow2 else lax.rem(me + n - j, n)

    def device(other):
        return {"tp": other // n_cp, "cp": lax.rem(other, n_cp)}

    def drain(ref, sem):
        pltpu.make_async_copy(ref, ref, sem).wait()

    index_copies = [
        pltpu.make_async_copy(ids_hbm, ids_ref, in_sem.at[nc + 1]),
        pltpu.make_async_copy(slot_hbm, slot_ref, in_sem.at[nc + 2]),
    ]
    for copy in index_copies:
        copy.start()
    tok_copies = []
    for c in range(nc):
        cols = pl.ds(c * dc, dc)
        copy = pltpu.make_async_copy(tok_hbm.at[:, cols], tok.at[:, cols], in_sem.at[c])
        copy.start()
        tok_copies.append(copy)
    rt_copy = pltpu.make_async_copy(rt_hbm, rt, in_sem.at[nc])
    rt_copy.start()

    barrier = pltpu.get_barrier_semaphore()
    for j in order:
        pl.semaphore_signal(barrier, inc=1, device_id=device(peer(j)), device_id_type=MESH)

    up_copies, down_copies = {}, {}
    for e in range(local):
        for c in range(nc):
            cols = pl.ds(c * dc, dc)
            pair = [
                pltpu.make_async_copy(wg_hbm.at[e, cols, :], wg.at[e, cols, :], wsem.at[0, e, c]),
                pltpu.make_async_copy(wu_hbm.at[e, cols, :], wu.at[e, cols, :], wsem.at[1, e, c]),
            ]
            for copy in pair:
                copy.start()
            up_copies[e, c] = pair
        for c in range(nc):
            cols = pl.ds(c * dc, dc)
            copy = pltpu.make_async_copy(wd_hbm.at[e, :, cols], wd.at[e, :, cols], wsem.at[2, e, c])
            copy.start()
            down_copies[e, c] = copy

    for copy in index_copies:
        copy.wait()
    ids0, ids1 = ids_ref[0:1, :], ids_ref[1:2, :]
    slot0, slot1 = slot_ref[0:1, :], slot_ref[1:2, :]
    target0 = jnp.where(slot0 >= 0, ids0 * CAP_DEV + slot0, -1)
    target1 = jnp.where(slot1 >= 0, ids1 * CAP_DEV + slot1, -1)
    row = lax.broadcasted_iota(jnp.int32, (slots, ids0.shape[1]), 0)
    placing = jnp.where((row == target0) | (row == target1), 1.0, 0.0).astype(jnp.bfloat16)

    half = my_z // h
    gateway = (my_z == inner[0]) | (my_z == inner[-1])
    pair = range(n_tp // h)
    near = [range(b * h, b * h + h) for b in pair]

    def place(e, c, z, x, recv_sem):
        pltpu.make_async_remote_copy(
            src_ref=xs.at[e, c, x],
            dst_ref=xr.at[e, c, me],
            send_sem=s1.at[e],
            recv_sem=recv_sem,
            device_id={"tp": jnp.int32(z), "cp": jnp.int32(x)},
            device_id_type=MESH,
        ).start()

    def cross(e, c):
        for b in pair if h < n_tp else ():
            for z in sorted(near[b], key=lambda z: z != inner[b]):
                ahead = half != b
                if z != inner[b] and relay[e] == 2:
                    continue
                if z != inner[b] and relay[e] == 1:
                    ahead = ahead & gateway
                @pl.when(ahead)
                def _():
                    for x in [lax.rem(my_x + i, n_cp) for i in range(1, n_cp + 1)]:
                        place(e, c, z, x, fr.at[e, c, lax.rem(me, h * n_cp)])

    def share(e, c):
        for z in range(n_tp):
            for x in range(n_cp):
                @pl.when((half == z // h) & (me != z * n_cp + x))
                def _():
                    place(e, c, z, x, r1.at[e, c])
        xr[e, c, me] = xs[e, c, my_x]

    def sources(b, e, outer):
        mine = inner[1 - b]
        return [
            z * n_cp + x
            for z in near[1 - b] if (z != mine) == outer
            for x in range(n_cp)
        ]

    def forward(e, c, outer):
        for b in pair if h < n_tp and relay[e] > (0 if outer else 1) else ():
            @pl.when(my_z == inner[b])
            def _():
                others = [z for z in near[b] if z != inner[b]]
                for k in sources(b, e, outer):
                    drain(xr.at[e, c, k], fr.at[e, c, k % (h * n_cp)])
                    for m, z in enumerate(others):
                        pltpu.make_async_remote_copy(
                            src_ref=xr.at[e, c, k],
                            dst_ref=xr.at[e, c, k],
                            send_sem=fs.at[e, m],
                            recv_sem=fr.at[e, c, k % (h * n_cp)],
                            device_id={"tp": jnp.int32(z), "cp": my_x},
                            device_id_type=MESH,
                        ).start()

    def collect(e, c):
        if h * n_cp > 1:
            drain(xr.at[e, c, pl.ds(0, h * n_cp - 1)], r1.at[e, c])
        for b in pair if h < n_tp else ():
            for outer in (False, True):
                late = half == b
                if relay[e] > (0 if outer else 1):
                    late = late & jnp.logical_not(gateway)
                @pl.when(late)
                def _():
                    for k in sources(b, e, outer):
                        drain(xr.at[e, c, k], fr.at[e, c, k % (h * n_cp)])

    for c in range(nc):
        tok_copies[c].wait()
        cols = pl.ds(c * dc, dc)
        outgoing = jnp.dot(placing, tok[:, cols], preferred_element_type=jnp.float32)
        for x in range(n_cp):
            for e in range(local):
                at = (x * local + e) * CAP_DEV
                xs[e, c, x] = outgoing[at:at + CAP_DEV].astype(jnp.bfloat16)
        if c == 0:
            pl.semaphore_wait(barrier, n - 1)
        if c == nc - 1:
            @pl.when(gateway)
            def _():
                for e in range(local):
                    for k in range(nc):
                        share(e, k)
                        cross(e, k)
            @pl.when(jnp.logical_not(gateway))
            def _():
                for step in (cross, share):
                    for e in range(local):
                        for k in range(nc):
                            step(e, k)

    rt_copy.wait()
    logits = lax.dot_general(rt[...], tok[...], NT, preferred_element_type=jnp.float32)
    affinity = 1.0 / (1.0 + jnp.exp(-logits))
    erow = lax.broadcasted_iota(jnp.int32, logits.shape, 0)
    chosen0 = jnp.sum(jnp.where(erow == ids0, affinity, 0.0), axis=0, keepdims=True)
    chosen1 = jnp.sum(jnp.where(erow == ids1, affinity, 0.0), axis=0, keepdims=True)
    total = chosen0 + chosen1
    share0 = ROUTE_SCALE * chosen0 / total
    share1 = ROUTE_SCALE * chosen1 / total
    wide = lax.broadcasted_iota(jnp.int32, (local * n * CAP_DEV, ids0.shape[1]), 0)
    which = lax.rem(wide // CAP_DEV, n_cp) * local + wide // (n * CAP_DEV)
    wide = which * CAP_DEV + lax.rem(wide, CAP_DEV)
    mix = jnp.where(wide == target0, share0, 0.0) + jnp.where(wide == target1, share1, 0.0)
    mix = mix.T
    mix_hi = mix.astype(jnp.bfloat16)
    mix_lo = (mix - mix_hi.astype(jnp.float32)).astype(jnp.bfloat16)
    mix_ref[...] = jnp.concatenate([mix_hi, mix_lo], axis=1)

    for e in range(local):
        for c in range(nc):
            forward(e, c, False)
            if e == 0 or EARLY:
                forward(e, c, True)
    rank = jnp.where(half == 0, my_z, my_z - h - 1)

    def merged(z, e):
        return h < n_tp and MERGE(z, h, e)

    def give_back(e, c, other):
        pltpu.make_async_remote_copy(
            src_ref=ps.at[e, c, other],
            dst_ref=pr.at[e, c, me],
            send_sem=s2,
            recv_sem=r2.at[e],
            device_id=device(jnp.int32(other)),
            device_id_type=MESH,
        ).start()

    for z in range(n_tp):
        for e in range(local):
            if merged(z, e):
                @pl.when(my_z == z)
                def _():
                    for k in sources(z // h, e, True):
                        for c in range(nc):
                            pr[e, c, k] = jnp.zeros(pr.shape[3:], pr.dtype)

    for e in range(local):
        gate = jnp.zeros((n * CAP_DEV, ff), jnp.float32)
        up = jnp.zeros((n * CAP_DEV, ff), jnp.float32)
        for c in range(nc):
            cols = pl.ds(c * dc, dc)
            for copy in up_copies[e, c]:
                copy.wait()
            collect(e, c)
            x = rows_of([xr[e, c, i] for i in range(n)])
            gate += jnp.dot(x, wg[e, cols, :], preferred_element_type=jnp.float32)
            up += jnp.dot(x, wu[e, cols, :], preferred_element_type=jnp.float32)
        for c in range(nc if e + 1 < local and not EARLY else 0):
            forward(e + 1, c, True)
        hidden = (gate / (1.0 + jnp.exp(-gate)) * up).astype(jnp.bfloat16)
        for c in range(nc):
            cols = pl.ds(c * dc, dc)
            down_copies[e, c].wait()
            part = jnp.dot(hidden, wd[e, :, cols], preferred_element_type=jnp.float32)
            turns = [z * n_cp + x for z in range(n_tp) for x in (reversed(range(n_cp)) if e < local - 1 else range(n_cp))]
            for other in turns:
                z = other // n_cp
                ps[e, c, other] = part[other * CAP_DEV:(other + 1) * CAP_DEV].astype(jnp.bfloat16)
                aside = z // h != half
                direct = other != me
                if merged(z, e):
                    direct = direct & jnp.logical_not(aside)
                @pl.when(direct)
                def _():
                    give_back(e, c, other)
                if merged(z, e):
                    at = other % (h * n_cp)
                    @pl.when(aside & gateway)
                    def _():
                        kept[e, c, at] = part[other * CAP_DEV:(other + 1) * CAP_DEV]
                    for b in pair:
                        if z // h == b:
                            continue
                        @pl.when((half == b) & jnp.logical_not(gateway))
                        def _():
                            pltpu.make_async_remote_copy(
                                src_ref=ps.at[e, c, other],
                                dst_ref=met.at[e, c, at, rank],
                                send_sem=s2,
                                recv_sem=ms.at[e],
                                device_id={"tp": jnp.int32(inner[b]), "cp": my_x},
                                device_id_type=MESH,
                            ).start()
            pr[e, c, me] = ps[e, c, me]
    for e in range(local):
        for b in pair if h < n_tp else ():
            ends = [z * n_cp + x for z in near[1 - b] if merged(z, e) for x in range(n_cp)]
            if not ends:
                continue
            @pl.when(my_z == inner[b])
            def _():
                drain(met.at[e, :, pl.ds(0, len(ends))], ms.at[e])
                for c in range(nc):
                    for other in ends:
                        at = other % (h * n_cp)
                        total = kept[e, c, at]
                        for m in range(h - 1):
                            total = total + met[e, c, at, m].astype(jnp.float32)
                        ps[e, c, other] = total.astype(jnp.bfloat16)
                        give_back(e, c, other)
    for e in range(local):
        own = h * n_cp - 1
        if h == n_tp or relay[e] == 0:
            drain(xr.at[e, :, pl.ds(0, n - 1)], s1.at[e])
            continue
        @pl.when(gateway)
        def _():
            drain(xr.at[e, :, pl.ds(0, own + (h * n_cp if relay[e] == 1 else n_cp))], s1.at[e])
            for m in range(h - 1):
                drain(xr.at[e, :, pl.ds(0, (h - 2 + relay[e]) * n_cp)], fs.at[e, m])
        @pl.when(jnp.logical_not(gateway))
        def _():
            drain(xr.at[e, :, pl.ds(0, own + n_cp)], s1.at[e])
    drain(pr.at[:, :, pl.ds(0, n - 1)], s2)
    for e in range(local):
        counts = [h * n_cp - 1 + n_cp if merged(z, e) else n - 1 for z in range(n_tp)]
        for count in sorted(set(counts)):
            here = [z for z in range(n_tp) if counts[z] == count]
            if len(here) == n_tp:
                drain(pr.at[e, :, pl.ds(0, count)], r2.at[e])
                continue
            @pl.when(functools.reduce(jnp.logical_or, [my_z == z for z in here]))
            def _():
                drain(pr.at[e, :, pl.ds(0, count)], r2.at[e])
        if e == local - 2:
            many = (local - 1) * n * CAP_DEV
            left = jnp.concatenate([mix_ref[:, :many], mix_ref[:, local * n * CAP_DEV:][:, :many]], axis=1)
            part = dc // SPLIT
            for c in range(nc):
                for p in range(SPLIT):
                    at = pl.ds(p * part, part)
                    rows = rows_of([pr[k, c, i, :, at] for k in range(e + 1) for i in range(n)])
                    rows = jnp.concatenate([rows, rows], axis=0)
                    base[:, pl.ds(c * dc + p * part, part)] = jnp.dot(
                        left, rows, preferred_element_type=jnp.float32
                    )
    if local == 1:
        base[...] = jnp.zeros_like(base)


def combine_kernel(pr, mix_ref, base, out_hbm, ob, osem):
    local, nc, n, cap, dc = pr.shape
    many, total = (local - 1) * n * cap, local * n * cap
    mix = jnp.concatenate([mix_ref[:, many:total], mix_ref[:, total + many:]], axis=1)
    part = dc // SPLIT
    outs = []
    for c in range(nc):
        for p in range(SPLIT):
            at = pl.ds(p * part, part)
            cols = pl.ds(c * dc + p * part, part)
            rows = rows_of([pr[e, c, i, :, at] for e in (local - 1,) for i in range(n)])
            rows = jnp.concatenate([rows, rows], axis=0)
            both = base[:, cols] + jnp.dot(mix, rows, preferred_element_type=jnp.float32)
            ob[:, cols] = both.astype(jnp.bfloat16)
            copy = pltpu.make_async_copy(ob.at[:, cols], out_hbm.at[:, cols], osem.at[c, p])
            copy.start()
            outs.append(copy)
    for copy in outs:
        copy.wait()


def body(n_tp, n_cp, tokens, router, gate_weight, up_weight, down_weight, expert_ids, slot_index):
    n = n_tp * n_cp
    rows, width = tokens.shape
    local, _, ff = gate_weight.shape
    nc = CHUNKS if n <= 16 else 1
    dc = width // nc
    anywhere = pl.BlockSpec(memory_space=pl.ANY)
    resident = pl.BlockSpec(memory_space=pltpu.VMEM)
    bf16 = jnp.bfloat16
    dma = pltpu.SemaphoreType.DMA
    slab = (local, nc, n, CAP_DEV, dc)
    across = max(n_tp // 2, 1) * n_cp
    pr, mix, base = pl.pallas_call(
        functools.partial(exchange_kernel, n_tp, n_cp, nc),
        out_shape=[
            pltpu.VMEM(slab, bf16),
            pltpu.VMEM((rows, 2 * local * n * CAP_DEV), bf16),
            pltpu.VMEM((rows, width), jnp.float32),
        ],
        in_specs=[anywhere] * 7,
        out_specs=[resident, resident, resident],
        scratch_shapes=[
            pltpu.VMEM((expert_ids.shape[1], rows), jnp.int32),
            pltpu.VMEM((slot_index.shape[1], rows), jnp.int32),
            pltpu.VMEM((rows, width), bf16),
            pltpu.VMEM((router.shape[1], width), bf16),
            pltpu.VMEM((local, width, ff), bf16),
            pltpu.VMEM((local, width, ff), bf16),
            pltpu.VMEM((local, ff, width), bf16),
            pltpu.VMEM((local, nc, n_cp, CAP_DEV, dc), bf16),
            pltpu.VMEM(slab, bf16),
            pltpu.VMEM(slab, bf16),
            pltpu.VMEM((local, nc, across, CAP_DEV, dc), jnp.float32),
            pltpu.VMEM((local, nc, across, max(n_tp // 2 - 1, 1), CAP_DEV, dc), bf16),
            dma((nc + 3,)),
            dma((3, local, nc)),
            dma((local,)),
            dma((local, nc)),
            dma((local, max(n_tp // 2 - 1, 1))),
            dma((local, nc, across)),
            dma,
            dma((local,)),
            dma((local,)),
        ],
        compiler_params=pltpu.CompilerParams(
            collective_id=0, has_side_effects=True, vmem_limit_bytes=60 * 1024 * 1024
        ),
    )(tokens, router.T, expert_ids.T, slot_index.T, gate_weight, up_weight, down_weight)
    return pl.pallas_call(
        combine_kernel,
        out_shape=jax.ShapeDtypeStruct((rows, width), bf16),
        in_specs=[resident, resident, resident],
        out_specs=anywhere,
        scratch_shapes=[
            pltpu.VMEM((rows, width), bf16),
            dma((nc, SPLIT)),
        ],
        compiler_params=pltpu.CompilerParams(vmem_limit_bytes=8 * 1024 * 1024),
    )(pr, mix, base)


def solution(mesh):
    in_specs = (
        P(("dp", "tp", "cp"), None),
        P(),
        P("cp", None, "tp"),
        P("cp", None, "tp"),
        P("cp", "tp", None),
        P(("dp", "tp", "cp"), None),
        P(("dp", "tp", "cp"), None),
    )
    out_specs = P(("dp", "tp", "cp"), None)
    step = functools.partial(body, mesh.shape["tp"], mesh.shape["cp"])
    return jax.shard_map(step, mesh=mesh, in_specs=in_specs, out_specs=out_specs, check_vma=False)
```
